512 devices in a mesh: mem: 32 (over y, x_hi, core), grid: 16 (over z, x_lo).
Axes of the slice: x: 4 (x_hi: 2, x_lo: 2; x = x_hi * 2 + x_lo), y: 8, z: 8, core: 2. Of those that a mesh axis runs over, the one named last changes fastest.
Arguments:
- ensemble: bfloat16 [64, 4, 128, 32, 128], P('mem', None, None, 'grid'), may hold values from -6 to 6
- control: bfloat16 [64, 128, 32, 128], P('mem', None, 'grid'), may hold values from -6 to 6
- vertical: bfloat16 [128, 128], replicated, may hold values from -0.5 to 0.5
- inverse_var: float32 [4, 128], replicated, may hold values from 0.25 to 4
- obs_code: int32 [64, 256], P('grid'), may hold values from 0 to 4
- obs_count: int32 [64, 256], P('grid'), may hold values from 0 to 3
Outputs:
- product: float32 [64, 128, 32, 128], P('mem', None, 'grid')
The draws below stay inside these ranges and needn't reach their ends.
All inputs are finite; a program needn't handle non-finite values.
Results may differ from the reference program's by a relative error of at most 0.00045.
Values sent between devices are 32-bit elements; how exact they have to be, the bound alone decides.
No kernel may reach another device: no remote copies, remote signals or barrier semaphores. Data moves between devices by JAX's collectives and lax.ppermute only.
A program may use at most 64 MiB of HBM per device.

```python
import math
import jax
import jax.numpy as jnp
from jax import lax

VARS = 4
LEV = 128
CY = 128
MEMBERS = 64
NX = 32


def place_ends(array, key, least, largest):
    dims = array.shape
    place = [jax.random.randint(jax.random.fold_in(key, axis), (), 0, dims[axis]) for axis in range(len(dims))]
    array = array.at[tuple(place)].set(least)
    longest = dims.index(max(dims))
    place[longest] = (place[longest] + 1) % dims[longest]
    return array.at[tuple(place)].set(largest)


def spiked(values, rng, source, target, blocks, factor):
    def block_of(axis_at):
        return (jnp.arange(values.shape[axis_at]) // (values.shape[axis_at] // blocks)).reshape((-1,) + (1,) * (values.ndim - 1 - axis_at))

    one_side = jax.random.permutation(rng, blocks)[block_of(target)]
    far = (block_of(target) + blocks // 2) % blocks
    return jnp.where((block_of(source) == one_side) | (block_of(source) == far), factor * values, values)


def block_scale(own_key, extent, cuts, smallest, top_value):
    def one(axis_at, blocks):
        heights = jax.random.uniform(jax.random.fold_in(jax.random.fold_in(own_key, 6), axis_at), (blocks,), jnp.float32, smallest / len(cuts), top_value / len(cuts))
        return jnp.repeat(jnp.exp(heights), extent[axis_at] // blocks).reshape((-1,) + (1,) * (len(extent) - axis_at - 1))

    level = one(*cuts[0])
    for cut in cuts[1:]:
        level = level * one(*cut)
    return level


def centred(own_key, extent, deviation, bound, pieces=(), dtype=jnp.bfloat16):
    array = deviation * jax.random.normal(own_key, extent, jnp.float32)
    if pieces:
        array = array * block_scale(own_key, extent, pieces, -0.22, 0.18)
    return jnp.clip(array, -bound, bound).astype(dtype)


def noise_with(key, dims, scale, reach, pieces, heavy, dtype=jnp.bfloat16):
    entries = scale * jax.random.normal(key, dims, jnp.float32)
    if pieces:
        entries = entries * block_scale(key, dims, pieces, -0.22, 0.18)
    return jnp.clip(spiked(entries, jax.random.fold_in(key, 3), *heavy), -reach, reach).astype(dtype)


def setup_inputs(seed: int = 0) -> dict:
    key_list = jax.random.split(jax.random.key(seed), 7)
    ensemble = noise_with(key_list[0], (MEMBERS, VARS, LEV, NX, CY), 1.0, 6.0, ((0, 32), (3, 16)), (0, 2, 32, 2.75))
    control = centred(key_list[1], (MEMBERS, LEV, NX, CY), 1.0, 6.0, ((0, 32), (2, 16)))
    vertical = centred(key_list[2], (LEV, LEV), LEV ** -0.5, 0.5)
    inverse_var = jnp.clip(jnp.exp(jax.random.uniform(key_list[3], (VARS, LEV), jnp.float32, math.log(0.25), math.log(4.0))), 0.25, 4.0)
    obs_code = place_ends(jax.random.randint(key_list[4], (2 * NX, 2 * CY), 0, 5), jax.random.fold_in(key_list[4], 1), 0, 4).astype(jnp.int32)
    obs_count = place_ends(jax.random.randint(key_list[5], (2 * NX, 2 * CY), 0, 4), jax.random.fold_in(key_list[5], 1), 0, 3).astype(jnp.int32)
    return dict(ensemble=ensemble, control=control, vertical=vertical, inverse_var=inverse_var, obs_code=obs_code, obs_count=obs_count)


diffusion = 0.2
near_weight = 0.75
far_weight = 0.25


def column_pair(field):
    padded = jnp.pad(field, [(0, 0)] * (field.ndim - 1) + [(1, 1)])
    return padded[..., 2:] + padded[..., :-2]


def row_margin(field):
    return jnp.pad(field, [(0, 0)] * (field.ndim - 2) + [(1, 1), (0, 0)])


def smooth_rows(extended):
    center = extended[..., 1:-1, :]
    return center + diffusion * (extended[..., 2:, :] + extended[..., :-2, :] + column_pair(center) - 4.0 * center)


def refine(coarse, extended):
    upper = near_weight * coarse + far_weight * extended[..., :-2, :]
    lower = near_weight * coarse + far_weight * extended[..., 2:, :]
    rows_fine = jnp.stack([upper, lower], axis=-2)
    rows_fine = rows_fine.reshape(coarse.shape[:-2] + (2 * coarse.shape[-2], coarse.shape[-1]))
    padded = jnp.pad(rows_fine, [(0, 0)] * (rows_fine.ndim - 1) + [(1, 1)])
    left = near_weight * rows_fine + far_weight * padded[..., :-2]
    right = near_weight * rows_fine + far_weight * padded[..., 2:]
    both = jnp.stack([left, right], axis=-1)
    return both.reshape(rows_fine.shape[:-1] + (2 * rows_fine.shape[-1],))


def coarsen(fine_field, extended):
    half_rows = fine_field.shape[-2] // 2
    rows_coarse = near_weight * (fine_field[..., 0::2, :] + fine_field[..., 1::2, :])
    rows_coarse = rows_coarse + far_weight * (extended[..., 0:2 * half_rows:2, :] + extended[..., 3::2, :])
    width = rows_coarse.shape[-1]
    padded = jnp.pad(rows_coarse, [(0, 0)] * (rows_coarse.ndim - 1) + [(1, 1)])
    result = near_weight * (rows_coarse[..., 0::2] + rows_coarse[..., 1::2])
    return result + far_weight * (padded[..., 0:width:2] + padded[..., 3::2])


def obs_masks(code):
    return [(code == which).astype(jnp.float32) for which in range(1, 5)]


def observe(fine_field, extended, masks, count, weights):
    padded = jnp.pad(fine_field, [(0, 0)] * (fine_field.ndim - 1) + [(1, 1)])
    diff = fine_field - masks[0] * extended[..., 2:, :] - masks[1] * extended[..., :-2, :]
    diff = diff - masks[2] * padded[..., 2:] - masks[3] * padded[..., :-2]
    return count.astype(jnp.float32) * weights[:, :, None, None] * diff


def adjoint_rows(forcing, masks, above, below):
    first = masks[0] * forcing
    second = masks[1] * forcing
    from_above = jnp.concatenate([above, first[..., :-1, :]], axis=-2)
    from_below = jnp.concatenate([second[..., 1:, :], below], axis=-2)
    pad_spec = [(0, 0)] * (forcing.ndim - 1) + [(1, 1)]
    from_left = jnp.pad(masks[2] * forcing, pad_spec)[..., :-2]
    from_right = jnp.pad(masks[3] * forcing, pad_spec)[..., 2:]
    return forcing - from_above - from_below - from_left - from_right


def smooth_twice(field):
    return smooth_rows(row_margin(smooth_rows(row_margin(field))))


def reference(ensemble, control, vertical, inverse_var, obs_code, obs_count):
    factor = MEMBERS ** -0.5
    vertical_wide = vertical.astype(jnp.float32)

    def accumulate(total, pair):
        member_pert, member_control = pair
        mixed = jnp.einsum("lm,mxy->lxy", vertical_wide, member_control.astype(jnp.float32), precision=lax.Precision.HIGHEST)
        local = smooth_twice(mixed)
        return total + factor * member_pert.astype(jnp.float32) * local[None], None

    increment, _ = lax.scan(accumulate, jnp.zeros((VARS, LEV, NX, CY), jnp.float32), (ensemble, control))
    fine_field = refine(increment, row_margin(increment))
    masks = obs_masks(obs_code)
    forcing = observe(fine_field, row_margin(fine_field), masks, obs_count, inverse_var)
    edge = jnp.zeros(forcing.shape[:-2] + (1, forcing.shape[-1]), jnp.float32)
    adjoint_fine = adjoint_rows(forcing, masks, edge, edge)
    adjoint = coarsen(adjoint_fine, row_margin(adjoint_fine))

    def gradient(pair):
        member_pert, member_control = pair
        projected = factor * jnp.sum(member_pert.astype(jnp.float32) * adjoint, axis=0)
        rounded = smooth_twice(projected).astype(jnp.bfloat16)
        back = jnp.einsum("ml,mxy->lxy", vertical_wide, rounded.astype(jnp.float32), precision=lax.Precision.HIGHEST)
        return member_control.astype(jnp.float32) + back

    return lax.map(gradient, (ensemble, control))
```

```python
import functools
import jax
import jax.numpy as jnp
from jax import lax
from jax.experimental import pallas as pl
from jax.experimental.pallas import tpu as pltpu
from jax.sharding import PartitionSpec as P

diffusion = 0.2
near_weight = 0.75
far_weight = 0.25

VMEM = pl.BlockSpec(memory_space=pltpu.VMEM)
SMEM = pl.BlockSpec(memory_space=pltpu.SMEM)
f32 = jnp.float32


def call(body, out_shapes, n_in, scratch=(), flops=1000000, scalars=1):
    return pl.pallas_call(
        body,
        out_shape=out_shapes,
        in_specs=[SMEM] * scalars + [VMEM] * (n_in - scalars),
        out_specs=jax.tree.map(lambda _: VMEM, out_shapes),
        scratch_shapes=list(scratch),
        compiler_params=pltpu.CompilerParams(vmem_limit_bytes=24 * 1024 * 1024),
        cost_estimate=pl.CostEstimate(flops=flops, bytes_accessed=1000000, transcendentals=0),
    )


def lanes(shape):
    return lax.broadcasted_iota(jnp.int32, shape, len(shape) - 1)


def from_left(x):
    return jnp.where(lanes(x.shape) == 0, 0.0, pltpu.roll(x, 1, x.ndim - 1))


def from_right(x):
    width = x.shape[-1]
    return jnp.where(lanes(x.shape) == width - 1, 0.0, pltpu.roll(x, width - 1, x.ndim - 1))


def smooth(row, up, down):
    pair = from_right(row) + from_left(row)
    return row + diffusion * (down + up + pair - 4.0 * row)


def smooth_twice(above, own, below, top, bottom):
    f_up = top * smooth(above[1], above[0], own[0])
    f_0 = smooth(own[0], above[1], own[1])
    f_1 = smooth(own[1], own[0], below[0])
    f_down = bottom * smooth(below[0], own[1], below[1])
    return smooth(f_0, f_up, f_1), smooth(f_1, f_0, f_down)


def rows_of(ref, start, count):
    return [ref[pl.ds(start + r, count, stride=2), :] for r in range(2)]


def neighbours(even, a, b):
    keep = even != 0
    return [jnp.where(keep, y, x) for x, y in zip(a, b)], [jnp.where(keep, x, y) for x, y in zip(a, b)]


def mix_kernel(control, vertical, code, count, out, wide):
    levels = vertical.shape[0]
    members = control.shape[0]
    for k in range(members):
        wide[...] = control[k].astype(f32)
        for r in range(2):
            row = wide[pl.ds(r, levels, stride=2), :].astype(jnp.bfloat16)
            out[pl.ds(2 * levels * k + r, levels, stride=2), :] = jnp.dot(
                vertical[...], row, preferred_element_type=f32
            )
    width = code.shape[1]
    source = lax.broadcasted_iota(jnp.int32, (width, width // 2), 0)
    target = lax.broadcasted_iota(jnp.int32, (width, width // 2), 1)
    at = 2 * levels * members
    n = code.shape[0]
    for i, what in enumerate((code, count)):
        values = what[...].astype(f32)
        for phase in range(2):
            pick = jnp.where(source == 2 * target + phase, 1.0, 0.0)
            out[pl.ds(at + (2 * i + phase) * n, n), :] = jnp.dot(
                values, pick, preferred_element_type=f32, precision=lax.Precision.HIGHEST
            )


def partial_kernel(factor, place, mixed, side_a, side_b, ensemble, keep, send, local):
    members, variables, height = ensemble.shape[:3]
    levels = height // 2
    even, top, bottom, first_core = (place[i] for i in range(4))
    for k in range(members):
        at = k * height
        above, below = neighbours(even, rows_of(side_a, at, levels), rows_of(side_b, at, levels))
        both = smooth_twice(
            above, rows_of(mixed, at, levels), below, top.astype(f32), bottom.astype(f32)
        )
        for r in range(2):
            local[k, pl.ds(r, levels, stride=2), :] = both[r]
    mine = first_core != 0
    for j in range(keep.shape[0]):
        at = pl.ds(16 * j, 16)
        fields = [local[k, at, :] for k in range(members)]
        for v in range(variables):
            total = ensemble[0, v, at, :].astype(f32) * fields[0]
            for k in range(1, members):
                total = total + ensemble[k, v, at, :].astype(f32) * fields[k]
            total = factor * total
            keep[j, v] = jnp.where(mine, total[:8], total[8:])
            send[j, v] = jnp.where(mine, total[8:], total[:8])


def pair_sum_kernel(place, keep, gathered, out):
    first = place[3] != 0
    for j in range(out.shape[0]):
        out[j] = keep[j] + jnp.where(first, gathered[1, j], gathered[0, j])


def total_kernel(arrived, out):
    total = arrived[0]
    for j in range(1, arrived.shape[0]):
        total = total + arrived[j]
    out[...] = total


def observe_kernel(place, share, swap_b, pair_a, meta, meta_a, meta_b, weights, out, rows):
    even, top, bottom = (place[i] for i in range(3))
    n = share.shape[0] // 2
    own = rows_of(share, 0, n)
    keep_even = even != 0
    a = [
        jnp.where(keep_even, pair_a[1, pl.ds(r, n, stride=2), :], pair_a[0, pl.ds(r, n, stride=2), :])
        for r in range(2)
    ]
    above, below = neighbours(even, a, rows_of(swap_b, 0, n))
    u = dict(zip(range(-2, 4), above + own + below))
    top, bottom = top.astype(f32), bottom.astype(f32)

    def inside(f):
        return top if f < 0 else bottom if f > 3 else None

    def masked(x, f):
        scale = inside(f)
        return x if scale is None else x * scale

    fine = {}
    for f in range(-3, 7):
        a_row = f // 2
        other = a_row - 1 if f % 2 == 0 else a_row + 1
        line = near_weight * u[a_row] + far_weight * u[other]
        fine[f] = [
            masked(near_weight * line + far_weight * from_left(line), f),
            masked(near_weight * line + far_weight * from_right(line), f),
        ]
    wanted_above, wanted_below = neighbours(even, [meta_a[...]], [meta_b[...]])
    table = [wanted_above[0], meta[...], wanted_below[0]]

    def lookup(which, phase, f):
        block, line = (f + 4) // 4, f % 4
        at = (2 * which + phase) * 4 + line
        return table[block][at : at + 1, :]

    scale = weights[...]
    forcing, first, second, third, fourth = {}, {}, {}, {}, {}
    for f in range(-2, 6):
        e, o = fine[f]
        nexts = (o, from_right(e))
        previous = (from_left(o), e)
        for phase in range(2):
            code = lookup(0, phase, f)
            count = lookup(1, phase, f)
            m = [(code == float(which)).astype(f32) for which in range(1, 5)]
            diff = fine[f][phase] - m[0] * fine[f + 1][phase] - m[1] * fine[f - 1][phase]
            diff = diff - m[2] * nexts[phase] - m[3] * previous[phase]
            value = count * scale * diff
            forcing[f, phase] = value
            first[f, phase] = m[0] * value
            second[f, phase] = m[1] * value
            third[f, phase] = m[2] * value
            fourth[f, phase] = m[3] * value
    adjoint = {}
    for f in range(-1, 5):
        came_left = (from_left(third[f, 1]), third[f, 0])
        came_right = (fourth[f, 1], from_right(fourth[f, 0]))
        for phase in range(2):
            value = forcing[f, phase] - first[f - 1, phase] - second[f + 1, phase]
            adjoint[f, phase] = masked(value - came_left[phase] - came_right[phase], f)
    for a_row in range(2):
        f = 2 * a_row
        e, o = (
            near_weight * (adjoint[f, p] + adjoint[f + 1, p])
            + far_weight * (adjoint[f - 1, p] + adjoint[f + 2, p])
            for p in range(2)
        )
        result = near_weight * (e + o) + far_weight * (from_left(o) + from_right(e))
        rows[pl.ds(a_row, n, stride=2), :] = result
    variables = out.shape[1]
    for v in range(variables):
        tile = rows[8 * v : 8 * v + 8, :]
        for j in range(out.shape[0]):
            out[j, v] = tile


def project_kernel(factor, adjoint, ensemble, out):
    members, variables, height = ensemble.shape[:3]
    for j in range(adjoint.shape[1]):
        at = pl.ds(16 * j, 16)
        for k in range(members):
            total = None
            for v in range(variables):
                wide = jnp.concatenate([adjoint[0, j, v], adjoint[1, j, v]], axis=0)
                term = ensemble[k, v, at, :].astype(f32) * wide
                total = term if total is None else total + term
            out[pl.ds(k * height + 16 * j, 16), :] = factor * total


def product_kernel(place, projected, side_a, side_b, control, transposed, out, wide):
    members, height = control.shape[:2]
    levels = height // 2
    even, top, bottom = (place[i] for i in range(3))
    for k in range(members):
        at = k * height
        above, below = neighbours(even, rows_of(side_a, at, levels), rows_of(side_b, at, levels))
        both = smooth_twice(
            above, rows_of(projected, at, levels), below, top.astype(f32), bottom.astype(f32)
        )
        wide[...] = control[k].astype(f32)
        for r in range(2):
            back = jnp.dot(
                transposed[...], both[r].astype(jnp.bfloat16), preferred_element_type=f32
            )
            out[k, pl.ds(r, levels, stride=2), :] = wide[pl.ds(r, levels, stride=2), :] + back


def per_device(ensemble, control, vertical, inverse_var, obs_code, obs_count):
    members, variables, levels, own_rows, width = ensemble.shape
    mem_size, grid_size = lax.axis_size("mem"), lax.axis_size("grid")
    factor = (members * mem_size) ** (-0.5)
    height = levels * own_rows
    half = mem_size // 2
    per_owner = levels // mem_size
    assert own_rows == 2 and per_owner * own_rows == 8
    mem_at, grid_at = lax.axis_index("mem"), lax.axis_index("grid")
    place = jnp.stack(
        [
            (grid_at % 2 == 0).astype(jnp.int32),
            (grid_at > 0).astype(jnp.int32),
            (grid_at < grid_size - 1).astype(jnp.int32),
            (mem_at % 2 == 0).astype(jnp.int32),
        ]
    )
    swap_a = [(i, i ^ 1) for i in range(grid_size)]
    swap_b = [(i, ((i + 1) ^ 1) - 1) for i in range(1, grid_size - 1)]
    pairs_a = [[2 * i, 2 * i + 1] for i in range(grid_size // 2)]
    cores = [[2 * i, 2 * i + 1] for i in range(half)]
    same_core = [[2 * i + c for i in range(half)] for c in range(2)]

    ens = ensemble.reshape(members, variables, height, width)
    ctl = control.reshape(members, height, width)
    meta_rows = 4 * obs_code.shape[0]
    sent_rows = members * height + meta_rows

    mixed = call(
        mix_kernel,
        jax.ShapeDtypeStruct((sent_rows, width), f32),
        4,
        [pltpu.VMEM((height, width), f32)],
        scalars=0,
    )(ctl, vertical, obs_code, obs_count)
    mixed_b = lax.ppermute(mixed, "grid", swap_b)
    mixed_a = lax.ppermute(mixed, "grid", swap_a)

    block = jax.ShapeDtypeStruct((half, variables, 8, width), f32)
    keep, send = call(
        functools.partial(partial_kernel, factor),
        (block, block),
        5,
        [pltpu.VMEM((members, height, width), f32)],
    )(place, mixed, mixed_a, mixed_b, ens)
    gathered = lax.all_gather(send, "mem", axis=0, axis_index_groups=cores)
    paired = call(pair_sum_kernel, block, 3)(place, keep, gathered)
    arrived = lax.all_to_all(paired, "mem", 0, 0, axis_index_groups=same_core, tiled=True)
    share = call(
        total_kernel, jax.ShapeDtypeStruct((variables, 8, width), f32), 1, scalars=0
    )(arrived).reshape(variables * 8, width)

    share_b = lax.ppermute(share, "grid", swap_b)
    share_a = lax.all_gather(share, "grid", axis=0, axis_index_groups=pairs_a)
    weights = lax.dynamic_slice_in_dim(inverse_var, mem_at * per_owner, per_owner, 1)
    weights = jnp.broadcast_to(weights.reshape(-1, 1), (variables * per_owner, width))
    meta, meta_a, meta_b = (x[members * height :] for x in (mixed, mixed_a, mixed_b))
    spread = call(
        observe_kernel, block, 8, [pltpu.VMEM((variables * 8, width), f32)]
    )(place, share, share_b, share_a, meta, meta_a, meta_b, weights)
    mine = lax.all_to_all(spread, "mem", 0, 0, axis_index_groups=same_core, tiled=True)
    adjoint = lax.all_gather(mine, "mem", axis=0, axis_index_groups=cores)

    projected = call(
        functools.partial(project_kernel, factor),
        jax.ShapeDtypeStruct((members * height, width), f32),
        2,
        scalars=0,
    )(adjoint, ens)
    projected_b = lax.ppermute(projected, "grid", swap_b)
    projected_a = lax.ppermute(projected, "grid", swap_a)
    out = call(
        product_kernel,
        jax.ShapeDtypeStruct((members, height, width), f32),
        6,
        [pltpu.VMEM((height, width), f32)],
    )(place, projected, projected_a, projected_b, ctl, vertical.T)
    return out.reshape(control.shape)


def solution(mesh):
    return jax.shard_map(
        per_device,
        mesh=mesh,
        in_specs=(
            P("mem", None, None, "grid", None),
            P("mem", None, "grid", None),
            P(),
            P(),
            P("grid", None),
            P("grid", None),
        ),
        out_specs=P("mem", None, "grid", None),
        check_vma=False,
    )
```

```python
import functools
import jax
import jax.numpy as jnp
from jax import lax
from jax.experimental import pallas as pl
from jax.experimental.pallas import tpu as pltpu
from jax.sharding import PartitionSpec as P

diffusion = 0.2
near_weight = 0.75
far_weight = 0.25

VMEM = pl.BlockSpec(memory_space=pltpu.VMEM)
SMEM = pl.BlockSpec(memory_space=pltpu.SMEM)
f32 = jnp.float32


ANY = pl.BlockSpec(memory_space=pl.ANY)


def call(body, out_shapes, in_specs, scratch=(), flops=1000000, out_spec=VMEM):
    return pl.pallas_call(
        body,
        out_shape=out_shapes,
        in_specs=list(in_specs),
        out_specs=jax.tree.map(lambda _: out_spec, out_shapes),
        scratch_shapes=list(scratch),
        compiler_params=pltpu.CompilerParams(vmem_limit_bytes=24 * 1024 * 1024),
        cost_estimate=pl.CostEstimate(flops=flops, bytes_accessed=1000000, transcendentals=0),
    )


def lanes(shape):
    return lax.broadcasted_iota(jnp.int32, shape, len(shape) - 1)


def from_left(x):
    return jnp.where(lanes(x.shape) == 0, 0.0, pltpu.roll(x, 1, x.ndim - 1))


def from_right(x):
    width = x.shape[-1]
    return jnp.where(lanes(x.shape) == width - 1, 0.0, pltpu.roll(x, width - 1, x.ndim - 1))


def smooth(row, up, down):
    pair = from_right(row) + from_left(row)
    return row + diffusion * (down + up + pair - 4.0 * row)


def smooth_twice(above, own, below, top, bottom):
    f_up = top * smooth(above[1], above[0], own[0])
    f_0 = smooth(own[0], above[1], own[1])
    f_1 = smooth(own[1], own[0], below[0])
    f_down = bottom * smooth(below[0], own[1], below[1])
    return smooth(f_0, f_up, f_1), smooth(f_1, f_0, f_down)


def rows_of(ref, start, count):
    return [ref[pl.ds(start + r, count, stride=2), :] for r in range(2)]


def neighbours(even, a, b):
    keep = even != 0
    return [jnp.where(keep, y, x) for x, y in zip(a, b)], [jnp.where(keep, x, y) for x, y in zip(a, b)]


def mix_kernel(control, vertical, out, wide):
    levels = vertical.shape[0]
    members = control.shape[0]
    for k in range(members):
        wide[...] = control[k].astype(f32)
        for r in range(2):
            row = wide[pl.ds(r, levels, stride=2), :].astype(jnp.bfloat16)
            out[pl.ds(2 * levels * k + r, levels, stride=2), :] = jnp.dot(
                vertical[...], row, preferred_element_type=f32
            )


def meta_kernel(after, code, count, ensemble, out):
    width = code.shape[1]
    source = lax.broadcasted_iota(jnp.int32, (width, width // 2), 0)
    target = lax.broadcasted_iota(jnp.int32, (width, width // 2), 1)
    n = code.shape[0]
    for i, what in enumerate((code, count)):
        values = what[...].astype(f32)
        for phase in range(2):
            pick = jnp.where(source == 2 * target + phase, 1.0, 0.0)
            out[pl.ds((2 * i + phase) * n, n), :] = jnp.dot(
                values, pick, preferred_element_type=f32, precision=lax.Precision.HIGHEST
            )


def partial_kernel(factor, place, after, mixed, side_a, side_b, ensemble, keep, send, local):
    members, variables, height = ensemble.shape[:3]
    levels = height // 2
    even, top, bottom, first_core = (place[i] for i in range(4))
    for k in range(members):
        at = k * height
        above, below = neighbours(even, rows_of(side_a, at, levels), rows_of(side_b, at, levels))
        both = smooth_twice(
            above, rows_of(mixed, at, levels), below, top.astype(f32), bottom.astype(f32)
        )
        for r in range(2):
            local[k, pl.ds(r, levels, stride=2), :] = both[r]
    mine = first_core != 0
    for j in range(keep.shape[0]):
        at = pl.ds(16 * j, 16)
        fields = [local[k, at, :] for k in range(members)]
        for v in range(variables):
            total = ensemble[0, v, at, :].astype(f32) * fields[0]
            for k in range(1, members):
                total = total + ensemble[k, v, at, :].astype(f32) * fields[k]
            total = factor * total
            keep[j, v] = jnp.where(mine, total[:8], total[8:])
            send[j, v] = jnp.where(mine, total[8:], total[:8])


def pair_sum_kernel(place, keep, gathered, out):
    first = place[3] != 0
    for j in range(out.shape[0]):
        out[j] = keep[j] + jnp.where(first, gathered[1, j], gathered[0, j])


def total_kernel(arrived, meta, out):
    total = arrived[0]
    for j in range(1, arrived.shape[0]):
        total = total + arrived[j]
    rows = 8 * total.shape[0]
    for v in range(total.shape[0]):
        out[8 * v : 8 * v + 8, :] = total[v]
    out[rows:, :] = meta[...]


def observe_kernel(place, share, swap_b, pair_a, weights, out, rows):
    even, top, bottom = (place[i] for i in range(3))
    height = rows.shape[0]
    n = height // 2
    own = rows_of(share, 0, n)
    keep_even = even != 0
    a = [
        jnp.where(keep_even, pair_a[1, pl.ds(r, n, stride=2), :], pair_a[0, pl.ds(r, n, stride=2), :])
        for r in range(2)
    ]
    above, below = neighbours(even, a, rows_of(swap_b, 0, n))
    u = dict(zip(range(-2, 4), above + own + below))
    top, bottom = top.astype(f32), bottom.astype(f32)

    def inside(f):
        return top if f < 0 else bottom if f > 3 else None

    def masked(x, f):
        scale = inside(f)
        return x if scale is None else x * scale

    fine = {}
    for f in range(-3, 7):
        a_row = f // 2
        other = a_row - 1 if f % 2 == 0 else a_row + 1
        line = near_weight * u[a_row] + far_weight * u[other]
        fine[f] = [
            masked(near_weight * line + far_weight * from_left(line), f),
            masked(near_weight * line + far_weight * from_right(line), f),
        ]
    meta_a = jnp.where(keep_even, pair_a[1, height:, :], pair_a[0, height:, :])
    wanted_above, wanted_below = neighbours(even, [meta_a], [swap_b[height:, :]])
    table = [wanted_above[0], share[height:, :], wanted_below[0]]

    def lookup(which, phase, f):
        block, line = (f + 4) // 4, f % 4
        at = (2 * which + phase) * 4 + line
        return table[block][at : at + 1, :]

    scale = weights[...]
    forcing, first, second, third, fourth = {}, {}, {}, {}, {}
    for f in range(-2, 6):
        e, o = fine[f]
        nexts = (o, from_right(e))
        previous = (from_left(o), e)
        for phase in range(2):
            code = lookup(0, phase, f)
            count = lookup(1, phase, f)
            m = [(code == float(which)).astype(f32) for which in range(1, 5)]
            diff = fine[f][phase] - m[0] * fine[f + 1][phase] - m[1] * fine[f - 1][phase]
            diff = diff - m[2] * nexts[phase] - m[3] * previous[phase]
            value = count * scale * diff
            forcing[f, phase] = value
            first[f, phase] = m[0] * value
            second[f, phase] = m[1] * value
            third[f, phase] = m[2] * value
            fourth[f, phase] = m[3] * value
    adjoint = {}
    for f in range(-1, 5):
        came_left = (from_left(third[f, 1]), third[f, 0])
        came_right = (fourth[f, 1], from_right(fourth[f, 0]))
        for phase in range(2):
            value = forcing[f, phase] - first[f - 1, phase] - second[f + 1, phase]
            adjoint[f, phase] = masked(value - came_left[phase] - came_right[phase], f)
    for a_row in range(2):
        f = 2 * a_row
        e, o = (
            near_weight * (adjoint[f, p] + adjoint[f + 1, p])
            + far_weight * (adjoint[f - 1, p] + adjoint[f + 2, p])
            for p in range(2)
        )
        result = near_weight * (e + o) + far_weight * (from_left(o) + from_right(e))
        rows[pl.ds(a_row, n, stride=2), :] = result
    variables = out.shape[1]
    for v in range(variables):
        tile = rows[8 * v : 8 * v + 8, :]
        for j in range(out.shape[0]):
            out[j, v] = tile


def project_kernel(factor, adjoint, ensemble, out):
    members, variables, height = ensemble.shape[:3]
    for j in range(adjoint.shape[1]):
        at = pl.ds(16 * j, 16)
        for k in range(members):
            total = None
            for v in range(variables):
                wide = jnp.concatenate([adjoint[0, j, v], adjoint[1, j, v]], axis=0)
                term = ensemble[k, v, at, :].astype(f32) * wide
                total = term if total is None else total + term
            out[pl.ds(k * height + 16 * j, 16), :] = factor * total


def product_kernel(place, projected, side_a, side_b, control, transposed, far, out, wide, sems):
    members, height = control.shape[:2]
    levels = height // 2
    even, top, bottom = (place[i] for i in range(3))
    for k in range(members):
        at = k * height
        above, below = neighbours(even, rows_of(side_a, at, levels), rows_of(side_b, at, levels))
        both = smooth_twice(
            above, rows_of(projected, at, levels), below, top.astype(f32), bottom.astype(f32)
        )
        wide[...] = control[k].astype(f32)
        for r in range(2):
            back = jnp.dot(
                transposed[...], both[r].astype(jnp.bfloat16), preferred_element_type=f32
            )
            out[k, pl.ds(r, levels, stride=2), :] = wide[pl.ds(r, levels, stride=2), :] + back
        pltpu.make_async_copy(out.at[k], far.at[k], sems.at[k]).start()
    for k in range(members):
        pltpu.make_async_copy(out.at[k], far.at[k], sems.at[k]).wait()


def per_device(ensemble, control, vertical, inverse_var, obs_code, obs_count):
    members, variables, levels, own_rows, width = ensemble.shape
    mem_size, grid_size = lax.axis_size("mem"), lax.axis_size("grid")
    factor = (members * mem_size) ** (-0.5)
    height = levels * own_rows
    half = mem_size // 2
    per_owner = levels // mem_size
    assert own_rows == 2 and per_owner * own_rows == 8
    mem_at, grid_at = lax.axis_index("mem"), lax.axis_index("grid")
    place = jnp.stack(
        [
            (grid_at % 2 == 0).astype(jnp.int32),
            (grid_at > 0).astype(jnp.int32),
            (grid_at < grid_size - 1).astype(jnp.int32),
            (mem_at % 2 == 0).astype(jnp.int32),
        ]
    )
    swap_a = [(i, i ^ 1) for i in range(grid_size)]
    swap_b = [(i, ((i + 1) ^ 1) - 1) for i in range(1, grid_size - 1)]
    pairs_a = [[2 * i, 2 * i + 1] for i in range(grid_size // 2)]
    cores = [[2 * i, 2 * i + 1] for i in range(half)]
    same_core = [[2 * i + c for i in range(half)] for c in range(2)]

    ens = ensemble.reshape(members, variables, height, width)
    ctl = control.reshape(members, height, width)
    meta_rows = 4 * obs_code.shape[0]

    mixed = call(
        mix_kernel,
        jax.ShapeDtypeStruct((members * height, width), f32),
        [VMEM, VMEM],
        [pltpu.VMEM((height, width), f32)],
    )(ctl, vertical)
    mixed_b = lax.ppermute(mixed, "grid", swap_b)
    mixed_a = lax.ppermute(mixed, "grid", swap_a)
    meta = call(
        meta_kernel, jax.ShapeDtypeStruct((meta_rows, width), f32), [ANY, VMEM, VMEM, VMEM]
    )(mixed, obs_code, obs_count, ens)
    weights = lax.dynamic_slice_in_dim(inverse_var, mem_at * per_owner, per_owner, 1)
    weights = jnp.broadcast_to(weights.reshape(-1, 1), (variables * per_owner, width))

    block = jax.ShapeDtypeStruct((half, variables, 8, width), f32)
    keep, send = call(
        functools.partial(partial_kernel, factor),
        (block, block),
        [SMEM, ANY] + [VMEM] * 4,
        [pltpu.VMEM((members, height, width), f32)],
    )(place, meta, mixed, mixed_a, mixed_b, ens)
    gathered = lax.all_gather(send, "mem", axis=0, axis_index_groups=cores)
    paired = call(pair_sum_kernel, block, [SMEM, VMEM, VMEM])(place, keep, gathered)
    turned = vertical.T
    paired, meta, weights, place, turned = lax.optimization_barrier(
        (paired, meta, weights, place, turned)
    )
    arrived = lax.all_to_all(paired, "mem", 0, 0, axis_index_groups=same_core, tiled=True)
    share = call(
        total_kernel, jax.ShapeDtypeStruct((variables * 8 + meta_rows, width), f32), [VMEM, VMEM]
    )(arrived, meta)

    share_b = lax.ppermute(share, "grid", swap_b)
    share_a = lax.all_gather(share, "grid", axis=0, axis_index_groups=pairs_a)
    spread = call(
        observe_kernel,
        block,
        [SMEM] + [VMEM] * 4,
        [pltpu.VMEM((variables * 8, width), f32)],
    )(place, share, share_b, share_a, weights)
    mine = lax.all_to_all(spread, "mem", 0, 0, axis_index_groups=same_core, tiled=True)
    adjoint = lax.all_gather(mine, "mem", axis=0, axis_index_groups=cores)

    projected = call(
        functools.partial(project_kernel, factor),
        jax.ShapeDtypeStruct((members * height, width), f32),
        [VMEM, VMEM],
    )(adjoint, ens)
    projected_b = lax.ppermute(projected, "grid", swap_b)
    projected_a = lax.ppermute(projected, "grid", swap_a)
    whole = jax.ShapeDtypeStruct((members, height, width), f32)
    out = call(
        product_kernel,
        whole,
        [SMEM] + [VMEM] * 5,
        [
            pltpu.VMEM(whole.shape, f32),
            pltpu.VMEM((height, width), f32),
            pltpu.SemaphoreType.DMA((members,)),
        ],
        out_spec=ANY,
    )(place, projected, projected_a, projected_b, ctl, turned)
    return out.reshape(control.shape)


def solution(mesh):
    return jax.shard_map(
        per_device,
        mesh=mesh,
        in_specs=(
            P("mem", None, None, "grid", None),
            P("mem", None, "grid", None),
            P(),
            P(),
            P("grid", None),
            P("grid", None),
        ),
        out_specs=P("mem", None, "grid", None),
        check_vma=False,
    )
```

```python
import functools
import jax
import jax.numpy as jnp
from jax import lax
from jax.experimental import pallas as pl
from jax.experimental.pallas import tpu as pltpu
from jax.sharding import PartitionSpec as P

diffusion = 0.2
near_weight = 0.75
far_weight = 0.25

VMEM = pl.BlockSpec(memory_space=pltpu.VMEM)
SMEM = pl.BlockSpec(memory_space=pltpu.SMEM)
f32 = jnp.float32


ANY = pl.BlockSpec(memory_space=pl.ANY)


def call(body, out_shapes, in_specs, scratch=(), flops=1000000, out_spec=VMEM):
    return pl.pallas_call(
        body,
        out_shape=out_shapes,
        in_specs=list(in_specs),
        out_specs=jax.tree.map(lambda _: out_spec, out_shapes),
        scratch_shapes=list(scratch),
        compiler_params=pltpu.CompilerParams(vmem_limit_bytes=24 * 1024 * 1024),
        cost_estimate=pl.CostEstimate(flops=flops, bytes_accessed=1000000, transcendentals=0),
    )


def lanes(shape):
    return lax.broadcasted_iota(jnp.int32, shape, len(shape) - 1)


def from_left(x):
    return jnp.where(lanes(x.shape) == 0, 0.0, pltpu.roll(x, 1, x.ndim - 1))


def from_right(x):
    width = x.shape[-1]
    return jnp.where(lanes(x.shape) == width - 1, 0.0, pltpu.roll(x, width - 1, x.ndim - 1))


def smooth(row, up, down):
    pair = from_right(row) + from_left(row)
    return row + diffusion * (down + up + pair - 4.0 * row)


def smooth_twice(above, own, below, top, bottom):
    f_up = top * smooth(above[1], above[0], own[0])
    f_0 = smooth(own[0], above[1], own[1])
    f_1 = smooth(own[1], own[0], below[0])
    f_down = bottom * smooth(below[0], own[1], below[1])
    return smooth(f_0, f_up, f_1), smooth(f_1, f_0, f_down)


def rows_of(ref, start, count):
    return [ref[pl.ds(start + r, count, stride=2), :] for r in range(2)]


def neighbours(even, a, b):
    keep = even != 0
    return [jnp.where(keep, y, x) for x, y in zip(a, b)], [jnp.where(keep, x, y) for x, y in zip(a, b)]


def halves(place, pair):
    mine = place[3] != 0
    return jnp.where(mine, pair[8:], pair[:8]), jnp.where(mine, pair[:8], pair[8:])


def mix_kernel(place, control, vertical, first, second, wide, mixed):
    levels = vertical.shape[0]
    members = control.shape[0]
    for k in range(members):
        wide[...] = control[k].astype(f32)
        for r in range(2):
            row = wide[pl.ds(r, levels, stride=2), :].astype(jnp.bfloat16)
            mixed[pl.ds(r, levels, stride=2), :] = jnp.dot(
                vertical[...], row, preferred_element_type=f32
            )
        for j in range(levels // 8):
            theirs, ours = halves(place, mixed[16 * j : 16 * j + 16, :])
            at = pl.ds(k * levels + 8 * j, 8)
            first[at, :] = theirs
            second[at, :] = ours


def meta_kernel(after, code, count, ensemble, out):
    width = code.shape[1]
    source = lax.broadcasted_iota(jnp.int32, (width, width // 2), 0)
    target = lax.broadcasted_iota(jnp.int32, (width, width // 2), 1)
    n = code.shape[0]
    for i, what in enumerate((code, count)):
        values = what[...].astype(f32)
        for phase in range(2):
            pick = jnp.where(source == 2 * target + phase, 1.0, 0.0)
            out[pl.ds((2 * i + phase) * n, n), :] = jnp.dot(
                values, pick, preferred_element_type=f32, precision=lax.Precision.HIGHEST
            )


def weighted(factor, place, which, rows, ensemble, local, finish):
    members, variables, height = ensemble.shape[:3]
    levels = height // 4
    even, top, bottom = (place[i] for i in range(3))
    own, side_a, side_b = rows
    for k in range(members):
        at = 2 * k * levels
        above, below = neighbours(even, rows_of(side_a, at, levels), rows_of(side_b, at, levels))
        both = smooth_twice(
            above, rows_of(own, at, levels), below, top.astype(f32), bottom.astype(f32)
        )
        for r in range(2):
            local[k, pl.ds(r, levels, stride=2), :] = both[r]
    for j in range(height // 16):
        for v in range(variables):
            total = None
            for k in range(members):
                pair = ensemble[k, v, 16 * j : 16 * j + 16, :].astype(f32)
                term = halves(place, pair)[which] * local[k, 8 * j : 8 * j + 8, :]
                total = term if total is None else total + term
            finish(j, v, factor * total)


def send_kernel(factor, place, after, own, side_a, side_b, ensemble, out, local):
    def finish(j, v, value):
        out[j, v] = value

    weighted(factor, place, 0, (own, side_a, side_b), ensemble, local, finish)


def keep_kernel(factor, place, own, side_a, side_b, ensemble, gathered, out, local):
    mine = place[3] != 0

    def finish(j, v, value):
        out[j, v] = value + jnp.where(mine, gathered[1, j, v], gathered[0, j, v])

    weighted(factor, place, 1, (own, side_a, side_b), ensemble, local, finish)


def total_kernel(arrived, meta, out):
    total = arrived[0]
    for j in range(1, arrived.shape[0]):
        total = total + arrived[j]
    rows = 8 * total.shape[0]
    for v in range(total.shape[0]):
        out[8 * v : 8 * v + 8, :] = total[v]
    out[rows:, :] = meta[...]


def observe_kernel(place, share, swap_b, pair_a, weights, out, rows):
    even, top, bottom = (place[i] for i in range(3))
    height = rows.shape[0]
    n = height // 2
    own = rows_of(share, 0, n)
    keep_even = even != 0
    a = [
        jnp.where(keep_even, pair_a[1, pl.ds(r, n, stride=2), :], pair_a[0, pl.ds(r, n, stride=2), :])
        for r in range(2)
    ]
    above, below = neighbours(even, a, rows_of(swap_b, 0, n))
    u = dict(zip(range(-2, 4), above + own + below))
    top, bottom = top.astype(f32), bottom.astype(f32)

    def inside(f):
        return top if f < 0 else bottom if f > 3 else None

    def masked(x, f):
        scale = inside(f)
        return x if scale is None else x * scale

    fine = {}
    for f in range(-3, 7):
        a_row = f // 2
        other = a_row - 1 if f % 2 == 0 else a_row + 1
        line = near_weight * u[a_row] + far_weight * u[other]
        fine[f] = [
            masked(near_weight * line + far_weight * from_left(line), f),
            masked(near_weight * line + far_weight * from_right(line), f),
        ]
    meta_a = jnp.where(keep_even, pair_a[1, height:, :], pair_a[0, height:, :])
    wanted_above, wanted_below = neighbours(even, [meta_a], [swap_b[height:, :]])
    table = [wanted_above[0], share[height:, :], wanted_below[0]]

    def lookup(which, phase, f):
        block, line = (f + 4) // 4, f % 4
        at = (2 * which + phase) * 4 + line
        return table[block][at : at + 1, :]

    scale = weights[...]
    forcing, first, second, third, fourth = {}, {}, {}, {}, {}
    for f in range(-2, 6):
        e, o = fine[f]
        nexts = (o, from_right(e))
        previous = (from_left(o), e)
        for phase in range(2):
            code = lookup(0, phase, f)
            count = lookup(1, phase, f)
            m = [(code == float(which)).astype(f32) for which in range(1, 5)]
            diff = fine[f][phase] - m[0] * fine[f + 1][phase] - m[1] * fine[f - 1][phase]
            diff = diff - m[2] * nexts[phase] - m[3] * previous[phase]
            value = count * scale * diff
            forcing[f, phase] = value
            first[f, phase] = m[0] * value
            second[f, phase] = m[1] * value
            third[f, phase] = m[2] * value
            fourth[f, phase] = m[3] * value
    adjoint = {}
    for f in range(-1, 5):
        came_left = (from_left(third[f, 1]), third[f, 0])
        came_right = (fourth[f, 1], from_right(fourth[f, 0]))
        for phase in range(2):
            value = forcing[f, phase] - first[f - 1, phase] - second[f + 1, phase]
            adjoint[f, phase] = masked(value - came_left[phase] - came_right[phase], f)
    for a_row in range(2):
        f = 2 * a_row
        e, o = (
            near_weight * (adjoint[f, p] + adjoint[f + 1, p])
            + far_weight * (adjoint[f - 1, p] + adjoint[f + 2, p])
            for p in range(2)
        )
        result = near_weight * (e + o) + far_weight * (from_left(o) + from_right(e))
        rows[pl.ds(a_row, n, stride=2), :] = result
    variables = out.shape[1]
    for v in range(variables):
        tile = rows[8 * v : 8 * v + 8, :]
        for j in range(out.shape[0]):
            out[j, v] = tile


def project(factor, place, which, tile, ensemble, out):
    members, variables, height = ensemble.shape[:3]
    for j in range(height // 16):
        tiles = [tile(j, v) for v in range(variables)]
        for k in range(members):
            total = None
            for v in range(variables):
                pair = ensemble[k, v, 16 * j : 16 * j + 16, :].astype(f32)
                term = halves(place, pair)[which] * tiles[v]
                total = term if total is None else total + term
            out[pl.ds(k * height // 2 + 8 * j, 8), :] = factor * total


def project_ours_kernel(factor, place, adjoint, ensemble, out):
    project(factor, place, 1, lambda j, v: adjoint[j, v], ensemble, out)


def project_theirs_kernel(factor, place, adjoint, ensemble, out):
    mine = place[3] != 0
    project(
        factor,
        place,
        0,
        lambda j, v: jnp.where(mine, adjoint[1, j, v], adjoint[0, j, v]),
        ensemble,
        out,
    )


def mixed_back(place, k, rows, turned):
    own, side_a, side_b = rows
    levels = turned.shape[1]
    even, top, bottom = (place[i] for i in range(3))
    at = 2 * k * levels
    above, below = neighbours(even, rows_of(side_a, at, levels), rows_of(side_b, at, levels))
    both = smooth_twice(
        above, rows_of(own, at, levels), below, top.astype(f32), bottom.astype(f32)
    )
    return [
        jnp.dot(turned[...], row.astype(jnp.bfloat16), preferred_element_type=f32) for row in both
    ]


def first_product_kernel(place, own, side_a, side_b, control, turned, out, wide):
    members, height = control.shape[:2]
    for k in range(members):
        back = mixed_back(place, k, (own, side_a, side_b), turned)
        wide[...] = control[k].astype(f32)
        for r in range(2):
            at = pl.ds(r, height // 2, stride=2)
            out[k, at, :] = wide[at, :] + back[r]


def second_product_kernel(place, own, side_a, side_b, started, turned, far, out, sems):
    members, height = started.shape[:2]
    for k in range(members):
        back = mixed_back(place, k, (own, side_a, side_b), turned)
        for r in range(2):
            at = pl.ds(r, height // 2, stride=2)
            out[k, at, :] = started[k, at, :] + back[r]
        pltpu.make_async_copy(out.at[k], far.at[k], sems.at[k]).start()
    for k in range(members):
        pltpu.make_async_copy(out.at[k], far.at[k], sems.at[k]).wait()


def per_device(ensemble, control, vertical, inverse_var, obs_code, obs_count):
    members, variables, levels, own_rows, width = ensemble.shape
    mem_size, grid_size = lax.axis_size("mem"), lax.axis_size("grid")
    factor = (members * mem_size) ** (-0.5)
    height = levels * own_rows
    half = mem_size // 2
    per_owner = levels // mem_size
    assert own_rows == 2 and per_owner * own_rows == 8
    mem_at, grid_at = lax.axis_index("mem"), lax.axis_index("grid")
    place = jnp.stack(
        [
            (grid_at % 2 == 0).astype(jnp.int32),
            (grid_at > 0).astype(jnp.int32),
            (grid_at < grid_size - 1).astype(jnp.int32),
            (mem_at % 2 == 0).astype(jnp.int32),
        ]
    )
    swap_a = [(i, i ^ 1) for i in range(grid_size)]
    swap_b = [(i, ((i + 1) ^ 1) - 1) for i in range(1, grid_size - 1)]
    pairs_a = [[2 * i, 2 * i + 1] for i in range(grid_size // 2)]
    cores = [[2 * i, 2 * i + 1] for i in range(half)]
    same_core = [[2 * i + c for i in range(half)] for c in range(2)]

    ens = ensemble.reshape(members, variables, height, width)
    ctl = control.reshape(members, height, width)
    meta_rows = 4 * obs_code.shape[0]

    def swapped(field):
        there_b = lax.ppermute(field, "grid", swap_b)
        return lax.ppermute(field, "grid", swap_a), there_b

    half_rows = jax.ShapeDtypeStruct((members * levels, width), f32)
    theirs, ours = call(
        mix_kernel,
        (half_rows, half_rows),
        [SMEM, VMEM, VMEM],
        [pltpu.VMEM((height, width), f32)] * 2,
    )(place, ctl, vertical)
    theirs_sides = swapped(theirs)
    ours_sides = swapped(ours)
    meta = call(
        meta_kernel, jax.ShapeDtypeStruct((meta_rows, width), f32), [ANY, VMEM, VMEM, VMEM]
    )(theirs, obs_code, obs_count, ens)
    weights = lax.dynamic_slice_in_dim(inverse_var, mem_at * per_owner, per_owner, 1)
    weights = jnp.broadcast_to(weights.reshape(-1, 1), (variables * per_owner, width))
    by_core = vertical.reshape(half, 2, per_owner, levels)
    turned_ours, turned_theirs = (
        lax.dynamic_index_in_dim(by_core, core, 1, False).reshape(levels // 2, levels).T
        for core in (mem_at % 2, 1 - mem_at % 2)
    )

    block = jax.ShapeDtypeStruct((half, variables, 8, width), f32)
    local = [pltpu.VMEM((members, levels, width), f32)]
    send = call(
        functools.partial(send_kernel, factor), block, [SMEM, ANY] + [VMEM] * 4, local
    )(place, meta, theirs, *theirs_sides, ens)
    gathered = lax.all_gather(send, "mem", axis=0, axis_index_groups=cores)
    paired = call(
        functools.partial(keep_kernel, factor), block, [SMEM] + [VMEM] * 5, local
    )(place, ours, *ours_sides, ens, gathered)
    paired, meta, weights, place, turned_ours, turned_theirs = lax.optimization_barrier(
        (paired, meta, weights, place, turned_ours, turned_theirs)
    )
    arrived = lax.all_to_all(paired, "mem", 0, 0, axis_index_groups=same_core, tiled=True)
    share = call(
        total_kernel, jax.ShapeDtypeStruct((variables * 8 + meta_rows, width), f32), [VMEM, VMEM]
    )(arrived, meta)

    share_b = lax.ppermute(share, "grid", swap_b)
    share_a = lax.all_gather(share, "grid", axis=0, axis_index_groups=pairs_a)
    spread = call(
        observe_kernel,
        block,
        [SMEM] + [VMEM] * 4,
        [pltpu.VMEM((variables * 8, width), f32)],
    )(place, share, share_b, share_a, weights)
    mine = lax.all_to_all(spread, "mem", 0, 0, axis_index_groups=same_core, tiled=True)

    ours = call(
        functools.partial(project_ours_kernel, factor), half_rows, [SMEM, VMEM, VMEM]
    )(place, mine, ens)
    ours, mine = lax.optimization_barrier((ours, mine))
    ours_sides = swapped(ours)
    adjoint = lax.all_gather(mine, "mem", axis=0, axis_index_groups=cores)
    theirs = call(
        functools.partial(project_theirs_kernel, factor), half_rows, [SMEM, VMEM, VMEM]
    )(place, adjoint, ens)
    theirs_sides = swapped(theirs)
    whole = jax.ShapeDtypeStruct((members, height, width), f32)
    started = call(
        first_product_kernel,
        whole,
        [SMEM] + [VMEM] * 5,
        [pltpu.VMEM((height, width), f32)],
    )(place, ours, *ours_sides, ctl, turned_ours)
    out = call(
        second_product_kernel,
        whole,
        [SMEM] + [VMEM] * 5,
        [pltpu.VMEM(whole.shape, f32), pltpu.SemaphoreType.DMA((members,))],
        out_spec=ANY,
    )(place, theirs, *theirs_sides, started, turned_theirs)
    return out.reshape(control.shape)


def solution(mesh):
    return jax.shard_map(
        per_device,
        mesh=mesh,
        in_specs=(
            P("mem", None, None, "grid", None),
            P("mem", None, "grid", None),
            P(),
            P(),
            P("grid", None),
            P("grid", None),
        ),
        out_specs=P("mem", None, "grid", None),
        check_vma=False,
    )
```

```python
import functools
import jax
import jax.numpy as jnp
from jax import lax
from jax.experimental import pallas as pl
from jax.experimental.pallas import tpu as pltpu
from jax.sharding import PartitionSpec as P

diffusion = 0.2
near_weight = 0.75
far_weight = 0.25

VMEM = pl.BlockSpec(memory_space=pltpu.VMEM)
SMEM = pl.BlockSpec(memory_space=pltpu.SMEM)
f32 = jnp.float32


ANY = pl.BlockSpec(memory_space=pl.ANY)


def call(body, out_shapes, in_specs, scratch=(), flops=1000000, out_spec=VMEM):
    return pl.pallas_call(
        body,
        out_shape=out_shapes,
        in_specs=list(in_specs),
        out_specs=jax.tree.map(lambda _: out_spec, out_shapes),
        scratch_shapes=list(scratch),
        compiler_params=pltpu.CompilerParams(vmem_limit_bytes=24 * 1024 * 1024),
        cost_estimate=pl.CostEstimate(flops=flops, bytes_accessed=1000000, transcendentals=0),
    )


def lanes(shape):
    return lax.broadcasted_iota(jnp.int32, shape, len(shape) - 1)


def from_left(x):
    return jnp.where(lanes(x.shape) == 0, 0.0, pltpu.roll(x, 1, x.ndim - 1))


def from_right(x):
    width = x.shape[-1]
    return jnp.where(lanes(x.shape) == width - 1, 0.0, pltpu.roll(x, width - 1, x.ndim - 1))


def smooth(row, up, down):
    pair = from_right(row) + from_left(row)
    return row + diffusion * (down + up + pair - 4.0 * row)


def smooth_twice(above, own, below, top, bottom):
    f_up = top * smooth(above[1], above[0], own[0])
    f_0 = smooth(own[0], above[1], own[1])
    f_1 = smooth(own[1], own[0], below[0])
    f_down = bottom * smooth(below[0], own[1], below[1])
    return smooth(f_0, f_up, f_1), smooth(f_1, f_0, f_down)


def own_part(own, top, bottom):
    zero = jnp.zeros_like(own[0])
    return smooth_twice((zero, zero), own, (zero, zero), top, bottom)


def halo_part(above, below, top, bottom):
    up = from_right(above[1]) + from_left(above[1])
    down = from_right(below[0]) + from_left(below[0])
    f_up = top * (above[1] + diffusion * (above[0] + up - 4.0 * above[1]))
    f_down = bottom * (below[0] + diffusion * (below[1] + down - 4.0 * below[0]))
    first = above[1] + diffusion * (up - 4.0 * above[1]) + f_up + diffusion * below[0]
    second = below[0] + diffusion * (down - 4.0 * below[0]) + f_down + diffusion * above[1]
    return diffusion * first, diffusion * second


def rows_of(ref, start, count):
    return [ref[pl.ds(start + r, count, stride=2), :] for r in range(2)]


def neighbours(even, a, b):
    keep = even != 0
    return [jnp.where(keep, y, x) for x, y in zip(a, b)], [jnp.where(keep, x, y) for x, y in zip(a, b)]


def mix_kernel(control, vertical, out, wide):
    levels = vertical.shape[0]
    members = control.shape[0]
    for k in range(members):
        wide[...] = control[k].astype(f32)
        for r in range(2):
            row = wide[pl.ds(r, levels, stride=2), :].astype(jnp.bfloat16)
            out[pl.ds(2 * levels * k + r, levels, stride=2), :] = jnp.dot(
                vertical[...], row, preferred_element_type=f32
            )


def meta_kernel(after, code, count, ensemble, out):
    width = code.shape[1]
    source = lax.broadcasted_iota(jnp.int32, (width, width // 2), 0)
    target = lax.broadcasted_iota(jnp.int32, (width, width // 2), 1)
    n = code.shape[0]
    for i, what in enumerate((code, count)):
        values = what[...].astype(f32)
        for phase in range(2):
            pick = jnp.where(source == 2 * target + phase, 1.0, 0.0)
            out[pl.ds((2 * i + phase) * n, n), :] = jnp.dot(
                values, pick, preferred_element_type=f32, precision=lax.Precision.HIGHEST
            )


def own_kernel(place, field, out):
    members, _, levels = out.shape[:3]
    top, bottom = place[1].astype(f32), place[2].astype(f32)
    for k in range(members):
        both = own_part(rows_of(field, 2 * k * levels, levels), top, bottom)
        for r in range(2):
            out[k, r] = both[r]


def own_control_kernel(place, field, control, vertical, out, wide, turned, spare):
    own_kernel(place, field, out)
    turned[...] = vertical[...].astype(f32).T.astype(turned.dtype)
    members, _, levels = out.shape[:3]
    for k in range(members):
        spare[...] = control[k].astype(f32)
        for r in range(2):
            wide[k, r] = spare[pl.ds(r, levels, stride=2), :]


def smoothed_rows(place, k, own, side_a, side_b):
    even, top, bottom = (place[i] for i in range(3))
    levels = own.shape[2]
    at = 2 * k * levels
    above, below = neighbours(even, rows_of(side_a, at, levels), rows_of(side_b, at, levels))
    both = halo_part(above, below, top.astype(f32), bottom.astype(f32))
    return [own[k, r] + both[r] for r in range(2)]


def partial_kernel(factor, place, after, own, side_a, side_b, ensemble, keep, send, local):
    members, variables, height = ensemble.shape[:3]
    levels = height // 2
    first_core = place[3]
    for k in range(members):
        both = smoothed_rows(place, k, own, side_a, side_b)
        for r in range(2):
            local[k, pl.ds(r, levels, stride=2), :] = both[r]
    mine = first_core != 0
    for j in range(keep.shape[0]):
        at = pl.ds(16 * j, 16)
        fields = [local[k, at, :] for k in range(members)]
        for v in range(variables):
            total = ensemble[0, v, at, :].astype(f32) * fields[0]
            for k in range(1, members):
                total = total + ensemble[k, v, at, :].astype(f32) * fields[k]
            total = factor * total
            keep[j, v] = jnp.where(mine, total[:8], total[8:])
            send[j, v] = jnp.where(mine, total[8:], total[:8])


def pair_sum_kernel(place, keep, gathered, out):
    first = place[3] != 0
    for j in range(out.shape[0]):
        out[j] = keep[j] + jnp.where(first, gathered[1, j], gathered[0, j])


def total_kernel(arrived, meta, out):
    total = arrived[0]
    for j in range(1, arrived.shape[0]):
        total = total + arrived[j]
    rows = 8 * total.shape[0]
    for v in range(total.shape[0]):
        out[8 * v : 8 * v + 8, :] = total[v]
    out[rows:, :] = meta[...]


def observe_kernel(place, inverse_var, share, swap_b, pair_a, out, rows):
    even, top, bottom = (place[i] for i in range(3))
    height = rows.shape[0]
    n = height // 2
    own = rows_of(share, 0, n)
    keep_even = even != 0
    a = [
        jnp.where(keep_even, pair_a[1, pl.ds(r, n, stride=2), :], pair_a[0, pl.ds(r, n, stride=2), :])
        for r in range(2)
    ]
    above, below = neighbours(even, a, rows_of(swap_b, 0, n))
    u = dict(zip(range(-2, 4), above + own + below))
    top, bottom = top.astype(f32), bottom.astype(f32)

    def inside(f):
        return top if f < 0 else bottom if f > 3 else None

    def masked(x, f):
        scale = inside(f)
        return x if scale is None else x * scale

    fine = {}
    for f in range(-3, 7):
        a_row = f // 2
        other = a_row - 1 if f % 2 == 0 else a_row + 1
        line = near_weight * u[a_row] + far_weight * u[other]
        fine[f] = [
            masked(near_weight * line + far_weight * from_left(line), f),
            masked(near_weight * line + far_weight * from_right(line), f),
        ]
    meta_a = jnp.where(keep_even, pair_a[1, height:, :], pair_a[0, height:, :])
    wanted_above, wanted_below = neighbours(even, [meta_a], [swap_b[height:, :]])
    table = [wanted_above[0], share[height:, :], wanted_below[0]]

    def lookup(which, phase, f):
        block, line = (f + 4) // 4, f % 4
        at = (2 * which + phase) * 4 + line
        return table[block][at : at + 1, :]

    variables = out.shape[1]
    per_owner = n // variables
    line = lax.broadcasted_iota(jnp.int32, own[0].shape, 0)
    scale = jnp.zeros(own[0].shape, f32)
    for v in range(variables):
        for l in range(per_owner):
            value = inverse_var[v, place[4] + l]
            scale = jnp.where(line == v * per_owner + l, value, scale)
    forcing, first, second, third, fourth = {}, {}, {}, {}, {}
    for f in range(-2, 6):
        e, o = fine[f]
        nexts = (o, from_right(e))
        previous = (from_left(o), e)
        for phase in range(2):
            code = lookup(0, phase, f)
            count = lookup(1, phase, f)
            m = [(code == float(which)).astype(f32) for which in range(1, 5)]
            diff = fine[f][phase] - m[0] * fine[f + 1][phase] - m[1] * fine[f - 1][phase]
            diff = diff - m[2] * nexts[phase] - m[3] * previous[phase]
            value = count * scale * diff
            forcing[f, phase] = value
            first[f, phase] = m[0] * value
            second[f, phase] = m[1] * value
            third[f, phase] = m[2] * value
            fourth[f, phase] = m[3] * value
    adjoint = {}
    for f in range(-1, 5):
        came_left = (from_left(third[f, 1]), third[f, 0])
        came_right = (fourth[f, 1], from_right(fourth[f, 0]))
        for phase in range(2):
            value = forcing[f, phase] - first[f - 1, phase] - second[f + 1, phase]
            adjoint[f, phase] = masked(value - came_left[phase] - came_right[phase], f)
    for a_row in range(2):
        f = 2 * a_row
        e, o = (
            near_weight * (adjoint[f, p] + adjoint[f + 1, p])
            + far_weight * (adjoint[f - 1, p] + adjoint[f + 2, p])
            for p in range(2)
        )
        result = near_weight * (e + o) + far_weight * (from_left(o) + from_right(e))
        rows[pl.ds(a_row, n, stride=2), :] = result
    for v in range(variables):
        tile = rows[8 * v : 8 * v + 8, :]
        for j in range(out.shape[0]):
            out[j, v] = tile


def project_kernel(factor, adjoint, ensemble, out):
    members, variables, height = ensemble.shape[:3]
    for j in range(adjoint.shape[1]):
        at = pl.ds(16 * j, 16)
        for k in range(members):
            total = None
            for v in range(variables):
                wide = jnp.concatenate([adjoint[0, j, v], adjoint[1, j, v]], axis=0)
                term = ensemble[k, v, at, :].astype(f32) * wide
                total = term if total is None else total + term
            out[pl.ds(k * height + 16 * j, 16), :] = factor * total


def product_kernel(place, own, side_a, side_b, control, transposed, far, out, sems):
    members, _, levels, width = control.shape
    for k in range(members):
        both = smoothed_rows(place, k, own, side_a, side_b)
        rounded = jnp.concatenate([row.astype(jnp.bfloat16) for row in both], axis=1)
        back = jnp.dot(transposed[...], rounded, preferred_element_type=f32)
        for r in range(2):
            out[k, pl.ds(r, levels, stride=2), :] = (
                control[k, r] + back[:, r * width : (r + 1) * width]
            )
        pltpu.make_async_copy(out.at[k], far.at[k], sems.at[k]).start()
    for k in range(members):
        pltpu.make_async_copy(out.at[k], far.at[k], sems.at[k]).wait()


def per_device(ensemble, control, vertical, inverse_var, obs_code, obs_count):
    members, variables, levels, own_rows, width = ensemble.shape
    mem_size, grid_size = lax.axis_size("mem"), lax.axis_size("grid")
    factor = (members * mem_size) ** (-0.5)
    height = levels * own_rows
    half = mem_size // 2
    per_owner = levels // mem_size
    assert own_rows == 2 and per_owner * own_rows == 8
    mem_at, grid_at = lax.axis_index("mem"), lax.axis_index("grid")
    place = jnp.stack(
        [
            (grid_at % 2 == 0).astype(jnp.int32),
            (grid_at > 0).astype(jnp.int32),
            (grid_at < grid_size - 1).astype(jnp.int32),
            (mem_at % 2 == 0).astype(jnp.int32),
            (mem_at * per_owner).astype(jnp.int32),
        ]
    )
    swap_a = [(i, i ^ 1) for i in range(grid_size)]
    swap_b = [(i, ((i + 1) ^ 1) - 1) for i in range(1, grid_size - 1)]
    pairs_a = [[2 * i, 2 * i + 1] for i in range(grid_size // 2)]
    cores = [[2 * i, 2 * i + 1] for i in range(half)]
    same_core = [[2 * i + c for i in range(half)] for c in range(2)]

    ens = ensemble.reshape(members, variables, height, width)
    ctl = control.reshape(members, height, width)
    meta_rows = 4 * obs_code.shape[0]

    mixed = call(
        mix_kernel,
        jax.ShapeDtypeStruct((members * height, width), f32),
        [VMEM, VMEM],
        [pltpu.VMEM((height, width), f32)],
    )(ctl, vertical)
    mixed_a = lax.ppermute(mixed, "grid", swap_a)
    mixed_b = lax.ppermute(mixed, "grid", swap_b)
    meta = call(
        meta_kernel, jax.ShapeDtypeStruct((meta_rows, width), f32), [ANY, VMEM, VMEM, VMEM]
    )(mixed, obs_code, obs_count, ens)
    own_shape = jax.ShapeDtypeStruct((members, own_rows, levels, width), f32)
    own = call(own_kernel, own_shape, [SMEM, VMEM])(place, mixed)

    block = jax.ShapeDtypeStruct((half, variables, 8, width), f32)
    keep, send = call(
        functools.partial(partial_kernel, factor),
        (block, block),
        [SMEM, ANY] + [VMEM] * 4,
        [pltpu.VMEM((members, height, width), f32)],
    )(place, meta, own, mixed_a, mixed_b, ens)
    gathered = lax.all_gather(send, "mem", axis=0, axis_index_groups=cores)
    paired = call(pair_sum_kernel, block, [SMEM, VMEM, VMEM])(place, keep, gathered)
    paired, meta, place = lax.optimization_barrier((paired, meta, place))
    arrived = lax.all_to_all(paired, "mem", 0, 0, axis_index_groups=same_core, tiled=True)
    share = call(
        total_kernel, jax.ShapeDtypeStruct((variables * 8 + meta_rows, width), f32), [VMEM, VMEM]
    )(arrived, meta)

    share_b = lax.ppermute(share, "grid", swap_b)
    share_a = lax.all_gather(share, "grid", axis=0, axis_index_groups=pairs_a)
    spread = call(
        observe_kernel,
        block,
        [SMEM, SMEM] + [VMEM] * 3,
        [pltpu.VMEM((variables * 8, width), f32)],
    )(place, inverse_var, share, share_b, share_a)
    mine = lax.all_to_all(spread, "mem", 0, 0, axis_index_groups=same_core, tiled=True)
    adjoint = lax.all_gather(mine, "mem", axis=0, axis_index_groups=cores)

    projected = call(
        functools.partial(project_kernel, factor),
        jax.ShapeDtypeStruct((members * height, width), f32),
        [VMEM, VMEM],
    )(adjoint, ens)
    projected_a = lax.ppermute(projected, "grid", swap_a)
    projected_b = lax.ppermute(projected, "grid", swap_b)
    own, wide, turned = call(
        own_control_kernel,
        (own_shape, own_shape, jax.ShapeDtypeStruct(vertical.shape, vertical.dtype)),
        [SMEM, VMEM, VMEM, VMEM],
        [pltpu.VMEM((height, width), f32)],
    )(place, projected, ctl, vertical)
    whole = jax.ShapeDtypeStruct((members, height, width), f32)
    out = call(
        product_kernel,
        whole,
        [SMEM] + [VMEM] * 5,
        [pltpu.VMEM(whole.shape, f32), pltpu.SemaphoreType.DMA((members,))],
        out_spec=ANY,
    )(place, own, projected_a, projected_b, wide, turned)
    return out.reshape(control.shape)


def solution(mesh):
    return jax.shard_map(
        per_device,
        mesh=mesh,
        in_specs=(
            P("mem", None, None, "grid", None),
            P("mem", None, "grid", None),
            P(),
            P(),
            P("grid", None),
            P("grid", None),
        ),
        out_specs=P("mem", None, "grid", None),
        check_vma=False,
    )
```

```python
import functools
import jax
import jax.numpy as jnp
from jax import lax
from jax.experimental import pallas as pl
from jax.experimental.pallas import tpu as pltpu
from jax.sharding import PartitionSpec as P

diffusion = 0.2
near_weight = 0.75
far_weight = 0.25

VMEM = pl.BlockSpec(memory_space=pltpu.VMEM)
f32 = jnp.float32


ANY = pl.BlockSpec(memory_space=pl.ANY)


def call(body, out_shapes, in_specs, scratch=(), flops=1000000, out_spec=VMEM):
    return pl.pallas_call(
        body,
        out_shape=out_shapes,
        in_specs=list(in_specs),
        out_specs=jax.tree.map(lambda _: out_spec, out_shapes),
        scratch_shapes=list(scratch),
        compiler_params=pltpu.CompilerParams(vmem_limit_bytes=24 * 1024 * 1024),
        cost_estimate=pl.CostEstimate(flops=flops, bytes_accessed=1000000, transcendentals=0),
    )


def lanes(shape):
    return lax.broadcasted_iota(jnp.int32, shape, len(shape) - 1)


def from_left(x):
    return jnp.where(lanes(x.shape) == 0, 0.0, pltpu.roll(x, 1, x.ndim - 1))


def from_right(x):
    width = x.shape[-1]
    return jnp.where(lanes(x.shape) == width - 1, 0.0, pltpu.roll(x, width - 1, x.ndim - 1))


def smooth(row, up, down):
    pair = from_right(row) + from_left(row)
    return row + diffusion * (down + up + pair - 4.0 * row)


def smooth_twice(above, own, below, top, bottom):
    f_up = top * smooth(above[1], above[0], own[0])
    f_0 = smooth(own[0], above[1], own[1])
    f_1 = smooth(own[1], own[0], below[0])
    f_down = bottom * smooth(below[0], own[1], below[1])
    return smooth(f_0, f_up, f_1), smooth(f_1, f_0, f_down)


def own_part(own, top, bottom):
    zero = jnp.zeros_like(own[0])
    return smooth_twice((zero, zero), own, (zero, zero), top, bottom)


def halo_part(above, below, top, bottom):
    up = from_right(above[1]) + from_left(above[1])
    down = from_right(below[0]) + from_left(below[0])
    f_up = top * (above[1] + diffusion * (above[0] + up - 4.0 * above[1]))
    f_down = bottom * (below[0] + diffusion * (below[1] + down - 4.0 * below[0]))
    first = above[1] + diffusion * (up - 4.0 * above[1]) + f_up + diffusion * below[0]
    second = below[0] + diffusion * (down - 4.0 * below[0]) + f_down + diffusion * above[1]
    return diffusion * first, diffusion * second


def rows_of(ref, start, count):
    return [ref[pl.ds(start + r, count, stride=2), :] for r in range(2)]


def neighbours(even, a, b):
    keep = even > 0.5
    return [jnp.where(keep, y, x) for x, y in zip(a, b)], [jnp.where(keep, x, y) for x, y in zip(a, b)]


def flags_of(place):
    return [place[i : i + 1, :] for i in range(4)]


def widen_kernel(control, out):
    members, height = control.shape[:2]
    for k in range(members):
        out[k * height : (k + 1) * height, :] = control[k].astype(f32)


def mixed_rows(vertical, fields):
    width = fields[0].shape[1]
    side_by_side = jnp.concatenate([x.astype(jnp.bfloat16) for x in fields], axis=1)
    product = jnp.dot(vertical[...], side_by_side, preferred_element_type=f32)
    return [product[:, i * width : (i + 1) * width] for i in range(len(fields))]


def meta_kernel(after, code, count, ensemble, out):
    width = code.shape[1]
    source = lax.broadcasted_iota(jnp.int32, (width, width // 2), 0)
    target = lax.broadcasted_iota(jnp.int32, (width, width // 2), 1)
    n = code.shape[0]
    for i, what in enumerate((code, count)):
        values = what[...].astype(f32)
        for phase in range(2):
            pick = jnp.where(source == 2 * target + phase, 1.0, 0.0)
            out[pl.ds((2 * i + phase) * n, n), :] = jnp.dot(
                values, pick, preferred_element_type=f32, precision=lax.Precision.HIGHEST
            )


def own_kernel(place, control, vertical, out):
    members, _, levels = out.shape[:3]
    _, top, bottom, _ = flags_of(place)
    for k in range(members):
        rows = mixed_rows(vertical, rows_of(control, 2 * k * levels, levels))
        both = own_part(rows, top, bottom)
        for r in range(2):
            out[k, r] = both[r]


def own_control_kernel(place, field, control, vertical, out, wide, turned, spare):
    turned[...] = vertical[...].astype(f32).T.astype(turned.dtype)
    members, _, levels = out.shape[:3]
    _, top, bottom, _ = flags_of(place)
    for k in range(members):
        both = own_part(rows_of(field, 2 * k * levels, levels), top, bottom)
        spare[...] = control[k].astype(f32)
        for r in range(2):
            out[k, r] = both[r]
            wide[k, r] = spare[pl.ds(r, levels, stride=2), :]


def smoothed_rows(place, k, own, side_a, side_b, vertical=None):
    even, top, bottom, _ = flags_of(place)
    levels = own.shape[2]
    at = 2 * k * levels
    above, below = neighbours(even, rows_of(side_a, at, levels), rows_of(side_b, at, levels))
    if vertical is not None:
        rows = mixed_rows(vertical, above + below)
        above, below = rows[:2], rows[2:]
    both = halo_part(above, below, top, bottom)
    return [own[k, r] + both[r] for r in range(2)]


def partial_kernel(
    factor, place, after, own, side_a, side_b, vertical, ensemble, keep, send, local
):
    members, variables, height = ensemble.shape[:3]
    levels = height // 2
    for k in range(members):
        both = smoothed_rows(place, k, own, side_a, side_b, vertical)
        for r in range(2):
            local[k, pl.ds(r, levels, stride=2), :] = both[r]
    mine = flags_of(place)[3] > 0.5
    for j in range(keep.shape[0]):
        at = pl.ds(16 * j, 16)
        fields = [local[k, at, :] for k in range(members)]
        for v in range(variables):
            total = ensemble[0, v, at, :].astype(f32) * fields[0]
            for k in range(1, members):
                total = total + ensemble[k, v, at, :].astype(f32) * fields[k]
            total = factor * total
            keep[j, v] = jnp.where(mine, total[:8], total[8:])
            send[j, v] = jnp.where(mine, total[8:], total[:8])


def pair_sum_kernel(place, keep, gathered, out):
    first = flags_of(place)[3] > 0.5
    for j in range(out.shape[0]):
        out[j] = keep[j] + jnp.where(first, gathered[1, j], gathered[0, j])


def total_kernel(arrived, meta, out):
    total = arrived[0]
    for j in range(1, arrived.shape[0]):
        total = total + arrived[j]
    rows = 8 * total.shape[0]
    for v in range(total.shape[0]):
        out[8 * v : 8 * v + 8, :] = total[v]
    out[rows:, :] = meta[...]


def observe_kernel(place, weights, share, swap_b, pair_a, out, rows):
    even, top, bottom, _ = flags_of(place)
    height = rows.shape[0]
    n = height // 2
    own = rows_of(share, 0, n)
    keep_even = even > 0.5
    a = [
        jnp.where(keep_even, pair_a[1, pl.ds(r, n, stride=2), :], pair_a[0, pl.ds(r, n, stride=2), :])
        for r in range(2)
    ]
    above, below = neighbours(even, a, rows_of(swap_b, 0, n))
    u = dict(zip(range(-2, 4), above + own + below))

    def inside(f):
        return top if f < 0 else bottom if f > 3 else None

    def masked(x, f):
        scale = inside(f)
        return x if scale is None else x * scale

    fine = {}
    for f in range(-3, 7):
        a_row = f // 2
        other = a_row - 1 if f % 2 == 0 else a_row + 1
        line = near_weight * u[a_row] + far_weight * u[other]
        fine[f] = [
            masked(near_weight * line + far_weight * from_left(line), f),
            masked(near_weight * line + far_weight * from_right(line), f),
        ]
    meta_a = jnp.where(keep_even, pair_a[1, height:, :], pair_a[0, height:, :])
    wanted_above, wanted_below = neighbours(even, [meta_a], [swap_b[height:, :]])
    table = [wanted_above[0], share[height:, :], wanted_below[0]]

    def lookup(which, phase, f):
        block, line = (f + 4) // 4, f % 4
        at = (2 * which + phase) * 4 + line
        return table[block][at : at + 1, :]

    scale = weights[...]
    forcing, first, second, third, fourth = {}, {}, {}, {}, {}
    for f in range(-2, 6):
        e, o = fine[f]
        nexts = (o, from_right(e))
        previous = (from_left(o), e)
        for phase in range(2):
            code = lookup(0, phase, f)
            count = lookup(1, phase, f)
            m = [(code == float(which)).astype(f32) for which in range(1, 5)]
            diff = fine[f][phase] - m[0] * fine[f + 1][phase] - m[1] * fine[f - 1][phase]
            diff = diff - m[2] * nexts[phase] - m[3] * previous[phase]
            value = count * scale * diff
            forcing[f, phase] = value
            first[f, phase] = m[0] * value
            second[f, phase] = m[1] * value
            third[f, phase] = m[2] * value
            fourth[f, phase] = m[3] * value
    adjoint = {}
    for f in range(-1, 5):
        came_left = (from_left(third[f, 1]), third[f, 0])
        came_right = (fourth[f, 1], from_right(fourth[f, 0]))
        for phase in range(2):
            value = forcing[f, phase] - first[f - 1, phase] - second[f + 1, phase]
            adjoint[f, phase] = masked(value - came_left[phase] - came_right[phase], f)
    for a_row in range(2):
        f = 2 * a_row
        e, o = (
            near_weight * (adjoint[f, p] + adjoint[f + 1, p])
            + far_weight * (adjoint[f - 1, p] + adjoint[f + 2, p])
            for p in range(2)
        )
        result = near_weight * (e + o) + far_weight * (from_left(o) + from_right(e))
        rows[pl.ds(a_row, n, stride=2), :] = result
    for v in range(out.shape[1]):
        tile = rows[8 * v : 8 * v + 8, :]
        for j in range(out.shape[0]):
            out[j, v] = tile


def project_kernel(factor, adjoint, ensemble, out):
    members, variables, height = ensemble.shape[:3]
    for j in range(adjoint.shape[1]):
        at = pl.ds(16 * j, 16)
        for k in range(members):
            total = None
            for v in range(variables):
                wide = jnp.concatenate([adjoint[0, j, v], adjoint[1, j, v]], axis=0)
                term = ensemble[k, v, at, :].astype(f32) * wide
                total = term if total is None else total + term
            out[pl.ds(k * height + 16 * j, 16), :] = factor * total


def product_kernel(place, own, side_a, side_b, control, transposed, far, out, sems):
    members, _, levels, width = control.shape
    for k in range(members):
        both = smoothed_rows(place, k, own, side_a, side_b)
        rounded = jnp.concatenate([row.astype(jnp.bfloat16) for row in both], axis=1)
        back = jnp.dot(transposed[...], rounded, preferred_element_type=f32)
        for r in range(2):
            out[k, pl.ds(r, levels, stride=2), :] = (
                control[k, r] + back[:, r * width : (r + 1) * width]
            )
        pltpu.make_async_copy(out.at[k], far.at[k], sems.at[k]).start()
    for k in range(members):
        pltpu.make_async_copy(out.at[k], far.at[k], sems.at[k]).wait()


def per_device(ensemble, control, vertical, inverse_var, obs_code, obs_count):
    members, variables, levels, own_rows, width = ensemble.shape
    mem_size, grid_size = lax.axis_size("mem"), lax.axis_size("grid")
    factor = (members * mem_size) ** (-0.5)
    height = levels * own_rows
    half = mem_size // 2
    per_owner = levels // mem_size
    assert own_rows == 2 and per_owner * own_rows == 8
    mem_at, grid_at = lax.axis_index("mem"), lax.axis_index("grid")
    flags = jnp.stack([grid_at % 2 == 0, grid_at > 0, grid_at < grid_size - 1, mem_at % 2 == 0])
    place = jnp.broadcast_to(jnp.pad(flags.astype(f32), (0, 4))[:, None], (8, width))
    weights = lax.dynamic_slice_in_dim(inverse_var, mem_at * per_owner, per_owner, 1)
    weights = jnp.broadcast_to(weights.reshape(-1, 1), (variables * per_owner, width))
    swap_a = [(i, i ^ 1) for i in range(grid_size)]
    swap_b = [(i, ((i + 1) ^ 1) - 1) for i in range(1, grid_size - 1)]
    pairs_a = [[2 * i, 2 * i + 1] for i in range(grid_size // 2)]
    cores = [[2 * i, 2 * i + 1] for i in range(half)]
    same_core = [[2 * i + c for i in range(half)] for c in range(2)]

    ens = ensemble.reshape(members, variables, height, width)
    ctl = control.reshape(members, height, width)
    meta_rows = 4 * obs_code.shape[0]

    field = jax.ShapeDtypeStruct((members * height, width), f32)
    wide = call(widen_kernel, field, [VMEM])(ctl)
    wide_a = lax.ppermute(wide, "grid", swap_a)
    wide_b = lax.ppermute(wide, "grid", swap_b)
    meta = call(
        meta_kernel, jax.ShapeDtypeStruct((meta_rows, width), f32), [ANY, VMEM, VMEM, VMEM]
    )(wide, obs_code, obs_count, ens)
    own_shape = jax.ShapeDtypeStruct((members, own_rows, levels, width), f32)
    own = call(own_kernel, own_shape, [VMEM] * 3)(place, wide, vertical)

    block = jax.ShapeDtypeStruct((half, variables, 8, width), f32)
    keep, send = call(
        functools.partial(partial_kernel, factor),
        (block, block),
        [VMEM, ANY] + [VMEM] * 5,
        [pltpu.VMEM((members, height, width), f32)],
    )(place, meta, own, wide_a, wide_b, vertical, ens)
    gathered = lax.all_gather(send, "mem", axis=0, axis_index_groups=cores)
    paired = call(pair_sum_kernel, block, [VMEM, VMEM, VMEM])(place, keep, gathered)
    paired, meta, place, weights = lax.optimization_barrier((paired, meta, place, weights))
    arrived = lax.all_to_all(paired, "mem", 0, 0, axis_index_groups=same_core, tiled=True)
    share = call(
        total_kernel, jax.ShapeDtypeStruct((variables * 8 + meta_rows, width), f32), [VMEM, VMEM]
    )(arrived, meta)

    share_b = lax.ppermute(share, "grid", swap_b)
    share_a = lax.all_gather(share, "grid", axis=0, axis_index_groups=pairs_a)
    spread = call(
        observe_kernel,
        block,
        [VMEM] * 5,
        [pltpu.VMEM((variables * 8, width), f32)],
    )(place, weights, share, share_b, share_a)
    mine = lax.all_to_all(spread, "mem", 0, 0, axis_index_groups=same_core, tiled=True)
    adjoint = lax.all_gather(mine, "mem", axis=0, axis_index_groups=cores)

    projected = call(
        functools.partial(project_kernel, factor),
        field,
        [VMEM, VMEM],
    )(adjoint, ens)
    projected_a = lax.ppermute(projected, "grid", swap_a)
    projected_b = lax.ppermute(projected, "grid", swap_b)
    own, wide, turned = call(
        own_control_kernel,
        (own_shape, own_shape, jax.ShapeDtypeStruct(vertical.shape, vertical.dtype)),
        [VMEM, VMEM, VMEM, VMEM],
        [pltpu.VMEM((height, width), f32)],
    )(place, projected, ctl, vertical)
    whole = jax.ShapeDtypeStruct((members, height, width), f32)
    out = call(
        product_kernel,
        whole,
        [VMEM] + [VMEM] * 5,
        [pltpu.VMEM(whole.shape, f32), pltpu.SemaphoreType.DMA((members,))],
        out_spec=ANY,
    )(place, own, projected_a, projected_b, wide, turned)
    return out.reshape(control.shape)


def solution(mesh):
    return jax.shard_map(
        per_device,
        mesh=mesh,
        in_specs=(
            P("mem", None, None, "grid", None),
            P("mem", None, "grid", None),
            P(),
            P(),
            P("grid", None),
            P("grid", None),
        ),
        out_specs=P("mem", None, "grid", None),
        check_vma=False,
    )
```

```python
import functools
import jax
import jax.numpy as jnp
from jax import lax
from jax.experimental import pallas as pl
from jax.experimental.pallas import tpu as pltpu
from jax.sharding import PartitionSpec as P

diffusion = 0.2
near_weight = 0.75
far_weight = 0.25

VMEM = pl.BlockSpec(memory_space=pltpu.VMEM)
f32 = jnp.float32


ANY = pl.BlockSpec(memory_space=pl.ANY)


def call(body, out_shapes, in_specs, scratch=(), flops=1000000, out_spec=VMEM):
    return pl.pallas_call(
        body,
        out_shape=out_shapes,
        in_specs=list(in_specs),
        out_specs=jax.tree.map(lambda _: out_spec, out_shapes),
        scratch_shapes=list(scratch),
        compiler_params=pltpu.CompilerParams(vmem_limit_bytes=24 * 1024 * 1024),
        cost_estimate=pl.CostEstimate(flops=flops, bytes_accessed=1000000, transcendentals=0),
    )


def lanes(shape):
    return lax.broadcasted_iota(jnp.int32, shape, len(shape) - 1)


def from_left(x):
    return jnp.where(lanes(x.shape) == 0, 0.0, pltpu.roll(x, 1, x.ndim - 1))


def from_right(x):
    width = x.shape[-1]
    return jnp.where(lanes(x.shape) == width - 1, 0.0, pltpu.roll(x, width - 1, x.ndim - 1))


def smooth(row, up, down):
    pair = from_right(row) + from_left(row)
    return row + diffusion * (down + up + pair - 4.0 * row)


def smooth_twice(above, own, below, top, bottom):
    f_up = top * smooth(above[1], above[0], own[0])
    f_0 = smooth(own[0], above[1], own[1])
    f_1 = smooth(own[1], own[0], below[0])
    f_down = bottom * smooth(below[0], own[1], below[1])
    return smooth(f_0, f_up, f_1), smooth(f_1, f_0, f_down)


def own_part(own, top, bottom):
    zero = jnp.zeros_like(own[0])
    return smooth_twice((zero, zero), own, (zero, zero), top, bottom)


def halo_part(above, below, top, bottom):
    up = from_right(above[1]) + from_left(above[1])
    down = from_right(below[0]) + from_left(below[0])
    f_up = top * (above[1] + diffusion * (above[0] + up - 4.0 * above[1]))
    f_down = bottom * (below[0] + diffusion * (below[1] + down - 4.0 * below[0]))
    first = above[1] + diffusion * (up - 4.0 * above[1]) + f_up + diffusion * below[0]
    second = below[0] + diffusion * (down - 4.0 * below[0]) + f_down + diffusion * above[1]
    return diffusion * first, diffusion * second


def rows_of(ref, start, count):
    return [ref[pl.ds(start + r, count, stride=2), :] for r in range(2)]


def neighbours(even, a, b):
    keep = even > 0.5
    return [jnp.where(keep, y, x) for x, y in zip(a, b)], [jnp.where(keep, x, y) for x, y in zip(a, b)]


def flags_of(place):
    return [place[i : i + 1, :] for i in range(4)]


def mixed_rows(vertical, fields):
    width = fields[0].shape[1]
    side_by_side = jnp.concatenate([x.astype(jnp.bfloat16) for x in fields], axis=1)
    product = jnp.dot(vertical[...], side_by_side, preferred_element_type=f32)
    return [product[:, i * width : (i + 1) * width] for i in range(len(fields))]


def meta_kernel(after, place, inverse_var, code, count, ensemble, out, weights):
    values = inverse_var[...]
    variables = values.shape[0]
    per_owner = weights.shape[0] // variables
    lane = lanes(values.shape).astype(f32)
    for l in range(per_owner):
        picked = jnp.where(lane == place[4:5, :] + float(l), values, 0.0)
        weights[pl.ds(l, variables, stride=per_owner), :] = jnp.broadcast_to(
            jnp.sum(picked, axis=1, keepdims=True), values.shape
        )
    width = code.shape[1]
    source = lax.broadcasted_iota(jnp.int32, (width, width // 2), 0)
    target = lax.broadcasted_iota(jnp.int32, (width, width // 2), 1)
    n = code.shape[0]
    for i, what in enumerate((code, count)):
        values = what[...].astype(f32)
        for phase in range(2):
            pick = jnp.where(source == 2 * target + phase, 1.0, 0.0)
            out[pl.ds((2 * i + phase) * n, n), :] = jnp.dot(
                values, pick, preferred_element_type=f32, precision=lax.Precision.HIGHEST
            )


def own_kernel(place, control, vertical, out):
    members, _, levels = out.shape[:3]
    _, top, bottom, _ = flags_of(place)
    for k in range(members):
        rows = mixed_rows(vertical, rows_of(control, 2 * k * levels, levels))
        both = own_part(rows, top, bottom)
        for r in range(2):
            out[k, r] = both[r]


def own_turned_kernel(place, field, vertical, out, turned):
    turned[...] = vertical[...].astype(f32).T.astype(turned.dtype)
    members, _, levels = out.shape[:3]
    _, top, bottom, _ = flags_of(place)
    for k in range(members):
        both = own_part(rows_of(field, 2 * k * levels, levels), top, bottom)
        for r in range(2):
            out[k, r] = both[r]


def smoothed_rows(place, k, own, side_a, side_b, vertical=None):
    even, top, bottom, _ = flags_of(place)
    levels = own.shape[2]
    at = 2 * k * levels
    above, below = neighbours(even, rows_of(side_a, at, levels), rows_of(side_b, at, levels))
    if vertical is not None:
        rows = mixed_rows(vertical, above + below)
        above, below = rows[:2], rows[2:]
    both = halo_part(above, below, top, bottom)
    return [own[k, r] + both[r] for r in range(2)]


def partial_kernel(
    factor, place, after, own, side_a, side_b, vertical, ensemble, keep, send, local
):
    members, variables, height = ensemble.shape[:3]
    levels = height // 2
    for k in range(members):
        both = smoothed_rows(place, k, own, side_a, side_b, vertical)
        for r in range(2):
            local[k, pl.ds(r, levels, stride=2), :] = both[r]
    mine = flags_of(place)[3] > 0.5
    for j in range(keep.shape[0]):
        at = pl.ds(16 * j, 16)
        fields = [local[k, at, :] for k in range(members)]
        for v in range(variables):
            total = ensemble[0, v, at, :].astype(f32) * fields[0]
            for k in range(1, members):
                total = total + ensemble[k, v, at, :].astype(f32) * fields[k]
            total = factor * total
            keep[j, v] = jnp.where(mine, total[:8], total[8:])
            send[j, v] = jnp.where(mine, total[8:], total[:8])


def pair_sum_kernel(place, keep, gathered, out):
    first = flags_of(place)[3] > 0.5
    for j in range(out.shape[0]):
        out[j] = keep[j] + jnp.where(first, gathered[1, j], gathered[0, j])


def total_kernel(arrived, meta, out):
    total = arrived[0]
    for j in range(1, arrived.shape[0]):
        total = total + arrived[j]
    rows = 8 * total.shape[0]
    for v in range(total.shape[0]):
        out[8 * v : 8 * v + 8, :] = total[v]
    out[rows:, :] = meta[...]


def observe_kernel(place, weights, share, swap_b, pair_a, out, rows):
    even, top, bottom, _ = flags_of(place)
    height = rows.shape[0]
    n = height // 2
    own = rows_of(share, 0, n)
    keep_even = even > 0.5
    a = [
        jnp.where(keep_even, pair_a[1, pl.ds(r, n, stride=2), :], pair_a[0, pl.ds(r, n, stride=2), :])
        for r in range(2)
    ]
    above, below = neighbours(even, a, rows_of(swap_b, 0, n))
    u = dict(zip(range(-2, 4), above + own + below))

    def inside(f):
        return top if f < 0 else bottom if f > 3 else None

    def masked(x, f):
        scale = inside(f)
        return x if scale is None else x * scale

    fine = {}
    for f in range(-3, 7):
        a_row = f // 2
        other = a_row - 1 if f % 2 == 0 else a_row + 1
        line = near_weight * u[a_row] + far_weight * u[other]
        fine[f] = [
            masked(near_weight * line + far_weight * from_left(line), f),
            masked(near_weight * line + far_weight * from_right(line), f),
        ]
    meta_a = jnp.where(keep_even, pair_a[1, height:, :], pair_a[0, height:, :])
    wanted_above, wanted_below = neighbours(even, [meta_a], [swap_b[height:, :]])
    table = [wanted_above[0], share[height:, :], wanted_below[0]]

    def lookup(which, phase, f):
        block, line = (f + 4) // 4, f % 4
        at = (2 * which + phase) * 4 + line
        return table[block][at : at + 1, :]

    scale = weights[...]
    forcing, first, second, third, fourth = {}, {}, {}, {}, {}
    for f in range(-2, 6):
        e, o = fine[f]
        nexts = (o, from_right(e))
        previous = (from_left(o), e)
        for phase in range(2):
            code = lookup(0, phase, f)
            count = lookup(1, phase, f)
            m = [(code == float(which)).astype(f32) for which in range(1, 5)]
            diff = fine[f][phase] - m[0] * fine[f + 1][phase] - m[1] * fine[f - 1][phase]
            diff = diff - m[2] * nexts[phase] - m[3] * previous[phase]
            value = count * scale * diff
            forcing[f, phase] = value
            first[f, phase] = m[0] * value
            second[f, phase] = m[1] * value
            third[f, phase] = m[2] * value
            fourth[f, phase] = m[3] * value
    adjoint = {}
    for f in range(-1, 5):
        came_left = (from_left(third[f, 1]), third[f, 0])
        came_right = (fourth[f, 1], from_right(fourth[f, 0]))
        for phase in range(2):
            value = forcing[f, phase] - first[f - 1, phase] - second[f + 1, phase]
            adjoint[f, phase] = masked(value - came_left[phase] - came_right[phase], f)
    for a_row in range(2):
        f = 2 * a_row
        e, o = (
            near_weight * (adjoint[f, p] + adjoint[f + 1, p])
            + far_weight * (adjoint[f - 1, p] + adjoint[f + 2, p])
            for p in range(2)
        )
        result = near_weight * (e + o) + far_weight * (from_left(o) + from_right(e))
        rows[pl.ds(a_row, n, stride=2), :] = result
    for v in range(out.shape[1]):
        tile = rows[8 * v : 8 * v + 8, :]
        for j in range(out.shape[0]):
            out[j, v] = tile


def project_kernel(factor, adjoint, ensemble, out):
    members, variables, height = ensemble.shape[:3]
    for j in range(adjoint.shape[1]):
        at = pl.ds(16 * j, 16)
        for k in range(members):
            total = None
            for v in range(variables):
                wide = jnp.concatenate([adjoint[0, j, v], adjoint[1, j, v]], axis=0)
                term = ensemble[k, v, at, :].astype(f32) * wide
                total = term if total is None else total + term
            out[pl.ds(k * height + 16 * j, 16), :] = factor * total


def product_kernel(place, own, side_a, side_b, control, transposed, far, out, sems):
    members, _, levels, width = own.shape
    for k in range(members):
        before = rows_of(control, 2 * k * levels, levels)
        both = smoothed_rows(place, k, own, side_a, side_b)
        rounded = jnp.concatenate([row.astype(jnp.bfloat16) for row in both], axis=1)
        back = jnp.dot(transposed[...], rounded, preferred_element_type=f32)
        for r in range(2):
            out[k, pl.ds(r, levels, stride=2), :] = (
                before[r] + back[:, r * width : (r + 1) * width]
            )
        pltpu.make_async_copy(out.at[k], far.at[k], sems.at[k]).start()
    for k in range(members):
        pltpu.make_async_copy(out.at[k], far.at[k], sems.at[k]).wait()


def per_device(ensemble, control, vertical, inverse_var, obs_code, obs_count):
    members, variables, levels, own_rows, width = ensemble.shape
    mem_size, grid_size = lax.axis_size("mem"), lax.axis_size("grid")
    factor = (members * mem_size) ** (-0.5)
    height = levels * own_rows
    half = mem_size // 2
    per_owner = levels // mem_size
    assert own_rows == 2 and per_owner * own_rows == 8
    mem_at, grid_at = lax.axis_index("mem"), lax.axis_index("grid")
    facts = [grid_at % 2 == 0, grid_at > 0, grid_at < grid_size - 1, mem_at % 2 == 0]
    facts = jnp.stack([x.astype(f32) for x in facts] + [(mem_at * per_owner).astype(f32)])
    place = jnp.broadcast_to(jnp.pad(facts, (0, 3))[:, None], (8, width))
    swap_a = [(i, i ^ 1) for i in range(grid_size)]
    swap_b = [(i, ((i + 1) ^ 1) - 1) for i in range(1, grid_size - 1)]
    pairs_a = [[2 * i, 2 * i + 1] for i in range(grid_size // 2)]
    cores = [[2 * i, 2 * i + 1] for i in range(half)]
    same_core = [[2 * i + c for i in range(half)] for c in range(2)]

    ens = ensemble.reshape(members, variables, height, width)
    ctl = control.reshape(members, height, width)
    meta_rows = 4 * obs_code.shape[0]

    field = jax.ShapeDtypeStruct((members * height, width), f32)
    wide = ctl.reshape(members * height, width).astype(f32)
    wide_a = lax.ppermute(wide, "grid", swap_a)
    wide_b = lax.ppermute(wide, "grid", swap_b)
    meta, weights = call(
        meta_kernel,
        (
            jax.ShapeDtypeStruct((meta_rows, width), f32),
            jax.ShapeDtypeStruct((variables * per_owner, width), f32),
        ),
        [ANY] + [VMEM] * 5,
    )(wide, place, inverse_var, obs_code, obs_count, ens)
    own_shape = jax.ShapeDtypeStruct((members, own_rows, levels, width), f32)
    own = call(own_kernel, own_shape, [VMEM] * 3)(place, wide, vertical)

    block = jax.ShapeDtypeStruct((half, variables, 8, width), f32)
    keep, send = call(
        functools.partial(partial_kernel, factor),
        (block, block),
        [VMEM, ANY] + [VMEM] * 5,
        [pltpu.VMEM((members, height, width), f32)],
    )(place, meta, own, wide_a, wide_b, vertical, ens)
    gathered = lax.all_gather(send, "mem", axis=0, axis_index_groups=cores)
    paired = call(pair_sum_kernel, block, [VMEM, VMEM, VMEM])(place, keep, gathered)
    paired, meta, place, weights = lax.optimization_barrier((paired, meta, place, weights))
    arrived = lax.all_to_all(paired, "mem", 0, 0, axis_index_groups=same_core, tiled=True)
    share = call(
        total_kernel, jax.ShapeDtypeStruct((variables * 8 + meta_rows, width), f32), [VMEM, VMEM]
    )(arrived, meta)

    share_b = lax.ppermute(share, "grid", swap_b)
    share_a = lax.all_gather(share, "grid", axis=0, axis_index_groups=pairs_a)
    spread = call(
        observe_kernel,
        block,
        [VMEM] * 5,
        [pltpu.VMEM((variables * 8, width), f32)],
    )(place, weights, share, share_b, share_a)
    mine = lax.all_to_all(spread, "mem", 0, 0, axis_index_groups=same_core, tiled=True)
    adjoint = lax.all_gather(mine, "mem", axis=0, axis_index_groups=cores)

    projected = call(
        functools.partial(project_kernel, factor),
        field,
        [VMEM, VMEM],
    )(adjoint, ens)
    projected_a = lax.ppermute(projected, "grid", swap_a)
    projected_b = lax.ppermute(projected, "grid", swap_b)
    own, turned = call(
        own_turned_kernel,
        (own_shape, jax.ShapeDtypeStruct(vertical.shape, vertical.dtype)),
        [VMEM] * 3,
    )(place, projected, vertical)
    whole = jax.ShapeDtypeStruct((members, height, width), f32)
    out = call(
        product_kernel,
        whole,
        [VMEM] + [VMEM] * 5,
        [pltpu.VMEM(whole.shape, f32), pltpu.SemaphoreType.DMA((members,))],
        out_spec=ANY,
    )(place, own, projected_a, projected_b, wide, turned)
    return out.reshape(control.shape)


def solution(mesh):
    return jax.shard_map(
        per_device,
        mesh=mesh,
        in_specs=(
            P("mem", None, None, "grid", None),
            P("mem", None, "grid", None),
            P(),
            P(),
            P("grid", None),
            P("grid", None),
        ),
        out_specs=P("mem", None, "grid", None),
        check_vma=False,
    )
```

```python
import functools
import jax
import jax.numpy as jnp
from jax import lax
from jax.experimental import pallas as pl
from jax.experimental.pallas import tpu as pltpu
from jax.sharding import PartitionSpec as P

diffusion = 0.2
near_weight = 0.75
far_weight = 0.25

VMEM = pl.BlockSpec(memory_space=pltpu.VMEM)
f32 = jnp.float32


ANY = pl.BlockSpec(memory_space=pl.ANY)


def call(body, out_shapes, in_specs, scratch=(), flops=1000000, out_spec=VMEM):
    return pl.pallas_call(
        body,
        out_shape=out_shapes,
        in_specs=list(in_specs),
        out_specs=jax.tree.map(lambda _: out_spec, out_shapes),
        scratch_shapes=list(scratch),
        compiler_params=pltpu.CompilerParams(vmem_limit_bytes=24 * 1024 * 1024),
        cost_estimate=pl.CostEstimate(flops=flops, bytes_accessed=1000000, transcendentals=0),
    )


def lanes(shape):
    return lax.broadcasted_iota(jnp.int32, shape, len(shape) - 1)


def from_left(x):
    return jnp.where(lanes(x.shape) == 0, 0.0, pltpu.roll(x, 1, x.ndim - 1))


def from_right(x):
    width = x.shape[-1]
    return jnp.where(lanes(x.shape) == width - 1, 0.0, pltpu.roll(x, width - 1, x.ndim - 1))


def smooth(row, up, down):
    pair = from_right(row) + from_left(row)
    return row + diffusion * (down + up + pair - 4.0 * row)


def smooth_twice(above, own, below, top, bottom):
    f_up = top * smooth(above[1], above[0], own[0])
    f_0 = smooth(own[0], above[1], own[1])
    f_1 = smooth(own[1], own[0], below[0])
    f_down = bottom * smooth(below[0], own[1], below[1])
    return smooth(f_0, f_up, f_1), smooth(f_1, f_0, f_down)


def own_part(own, top, bottom):
    zero = jnp.zeros_like(own[0])
    return smooth_twice((zero, zero), own, (zero, zero), top, bottom)


def halo_part(above, below, top, bottom):
    up = from_right(above[1]) + from_left(above[1])
    down = from_right(below[0]) + from_left(below[0])
    f_up = top * (above[1] + diffusion * (above[0] + up - 4.0 * above[1]))
    f_down = bottom * (below[0] + diffusion * (below[1] + down - 4.0 * below[0]))
    first = above[1] + diffusion * (up - 4.0 * above[1]) + f_up + diffusion * below[0]
    second = below[0] + diffusion * (down - 4.0 * below[0]) + f_down + diffusion * above[1]
    return diffusion * first, diffusion * second


def rows_of(ref, start, count):
    return [ref[pl.ds(start + r, count, stride=2), :] for r in range(2)]


def neighbours(even, a, b):
    keep = even > 0.5
    return [jnp.where(keep, y, x) for x, y in zip(a, b)], [jnp.where(keep, x, y) for x, y in zip(a, b)]


def flags_of(place):
    return [place[i : i + 1, :] for i in range(4)]


def mixed_rows(vertical, fields):
    width = fields[0].shape[1]
    side_by_side = jnp.concatenate([x.astype(jnp.bfloat16) for x in fields], axis=1)
    product = jnp.dot(vertical[...], side_by_side, preferred_element_type=f32)
    return [product[:, i * width : (i + 1) * width] for i in range(len(fields))]


def meta_kernel(after, place, inverse_var, code, count, ensemble, out, weights):
    values = inverse_var[...]
    variables = values.shape[0]
    per_owner = weights.shape[0] // variables
    lane = lanes(values.shape).astype(f32)
    for l in range(per_owner):
        picked = jnp.where(lane == place[4:5, :] + float(l), values, 0.0)
        weights[pl.ds(l, variables, stride=per_owner), :] = jnp.broadcast_to(
            jnp.sum(picked, axis=1, keepdims=True), values.shape
        )
    width = code.shape[1]
    source = lax.broadcasted_iota(jnp.int32, (width, width // 2), 0)
    target = lax.broadcasted_iota(jnp.int32, (width, width // 2), 1)
    n = code.shape[0]
    for i, what in enumerate((code, count)):
        values = what[...].astype(f32)
        for phase in range(2):
            pick = jnp.where(source == 2 * target + phase, 1.0, 0.0)
            out[pl.ds((2 * i + phase) * n, n), :] = jnp.dot(
                values, pick, preferred_element_type=f32, precision=lax.Precision.HIGHEST
            )


def own_kernel(place, control, vertical, out):
    members, _, levels = out.shape[:3]
    _, top, bottom, _ = flags_of(place)
    for k in range(members):
        rows = mixed_rows(vertical, rows_of(control, 2 * k * levels, levels))
        both = own_part(rows, top, bottom)
        for r in range(2):
            out[k, r] = both[r]


def own_turned_kernel(place, field, vertical, out, turned):
    turned[...] = vertical[...].astype(f32).T.astype(turned.dtype)
    members, _, levels = out.shape[:3]
    _, top, bottom, _ = flags_of(place)
    for k in range(members):
        both = own_part(rows_of(field, 2 * k * levels, levels), top, bottom)
        for r in range(2):
            out[k, r] = both[r]


def smoothed_rows(place, k, own, side_a, side_b, vertical=None):
    even, top, bottom, _ = flags_of(place)
    levels = own.shape[2]
    at = 2 * k * levels
    above, below = neighbours(even, rows_of(side_a, at, levels), rows_of(side_b, at, levels))
    if vertical is not None:
        rows = mixed_rows(vertical, above + below)
        above, below = rows[:2], rows[2:]
    both = halo_part(above, below, top, bottom)
    return [own[k, r] + both[r] for r in range(2)]


def partial_kernel(
    factor, place, after, own, side_a, side_b, vertical, ensemble, keep, send, local
):
    members, variables, height = ensemble.shape[:3]
    levels = height // 2
    for k in range(members):
        both = smoothed_rows(place, k, own, side_a, side_b, vertical)
        for r in range(2):
            local[k, pl.ds(r, levels, stride=2), :] = both[r]
    mine = flags_of(place)[3] > 0.5
    for j in range(keep.shape[0]):
        at = pl.ds(16 * j, 16)
        fields = [local[k, at, :] for k in range(members)]
        for v in range(variables):
            total = ensemble[0, v, at, :].astype(f32) * fields[0]
            for k in range(1, members):
                total = total + ensemble[k, v, at, :].astype(f32) * fields[k]
            total = factor * total
            keep[j, v] = jnp.where(mine, total[:8], total[8:])
            send[j, v] = jnp.where(mine, total[8:], total[:8])


def pair_sum_kernel(place, keep, gathered, out):
    first = flags_of(place)[3] > 0.5
    for j in range(out.shape[0]):
        out[j] = keep[j] + jnp.where(first, gathered[1, j], gathered[0, j])


def total_kernel(arrived, meta, out):
    total = arrived[0]
    for j in range(1, arrived.shape[0]):
        total = total + arrived[j]
    rows = 8 * total.shape[0]
    for v in range(total.shape[0]):
        out[8 * v : 8 * v + 8, :] = total[v]
    out[rows:, :] = meta[...]


def observe_kernel(place, weights, share, swap_b, swap_a, out, rows):
    even, top, bottom, _ = flags_of(place)
    height = rows.shape[0]
    n = height // 2
    own = rows_of(share, 0, n)
    above, below = neighbours(even, rows_of(swap_a, 0, n), rows_of(swap_b, 0, n))
    u = dict(zip(range(-2, 4), above + own + below))

    def inside(f):
        return top if f < 0 else bottom if f > 3 else None

    def masked(x, f):
        scale = inside(f)
        return x if scale is None else x * scale

    fine = {}
    for f in range(-3, 7):
        a_row = f // 2
        other = a_row - 1 if f % 2 == 0 else a_row + 1
        line = near_weight * u[a_row] + far_weight * u[other]
        fine[f] = [
            masked(near_weight * line + far_weight * from_left(line), f),
            masked(near_weight * line + far_weight * from_right(line), f),
        ]
    wanted_above, wanted_below = neighbours(even, [swap_a[height:, :]], [swap_b[height:, :]])
    table = [wanted_above[0], share[height:, :], wanted_below[0]]

    def lookup(which, phase, f):
        block, line = (f + 4) // 4, f % 4
        at = (2 * which + phase) * 4 + line
        return table[block][at : at + 1, :]

    scale = weights[...]
    forcing, first, second, third, fourth = {}, {}, {}, {}, {}
    for f in range(-2, 6):
        e, o = fine[f]
        nexts = (o, from_right(e))
        previous = (from_left(o), e)
        for phase in range(2):
            code = lookup(0, phase, f)
            count = lookup(1, phase, f)
            m = [(code == float(which)).astype(f32) for which in range(1, 5)]
            diff = fine[f][phase] - m[0] * fine[f + 1][phase] - m[1] * fine[f - 1][phase]
            diff = diff - m[2] * nexts[phase] - m[3] * previous[phase]
            value = count * scale * diff
            forcing[f, phase] = value
            first[f, phase] = m[0] * value
            second[f, phase] = m[1] * value
            third[f, phase] = m[2] * value
            fourth[f, phase] = m[3] * value
    adjoint = {}
    for f in range(-1, 5):
        came_left = (from_left(third[f, 1]), third[f, 0])
        came_right = (fourth[f, 1], from_right(fourth[f, 0]))
        for phase in range(2):
            value = forcing[f, phase] - first[f - 1, phase] - second[f + 1, phase]
            adjoint[f, phase] = masked(value - came_left[phase] - came_right[phase], f)
    for a_row in range(2):
        f = 2 * a_row
        e, o = (
            near_weight * (adjoint[f, p] + adjoint[f + 1, p])
            + far_weight * (adjoint[f - 1, p] + adjoint[f + 2, p])
            for p in range(2)
        )
        result = near_weight * (e + o) + far_weight * (from_left(o) + from_right(e))
        rows[pl.ds(a_row, n, stride=2), :] = result
    for v in range(out.shape[1]):
        tile = rows[8 * v : 8 * v + 8, :]
        for j in range(out.shape[0]):
            out[j, v] = tile


def project_kernel(factor, adjoint, ensemble, out):
    members, variables, height = ensemble.shape[:3]
    for j in range(adjoint.shape[1]):
        at = pl.ds(16 * j, 16)
        for k in range(members):
            total = None
            for v in range(variables):
                wide = jnp.concatenate([adjoint[0, j, v], adjoint[1, j, v]], axis=0)
                term = ensemble[k, v, at, :].astype(f32) * wide
                total = term if total is None else total + term
            out[pl.ds(k * height + 16 * j, 16), :] = factor * total


def product_kernel(place, own, side_a, side_b, control, transposed, far, out, sems):
    members, _, levels, width = own.shape
    for k in range(members):
        before = rows_of(control, 2 * k * levels, levels)
        both = smoothed_rows(place, k, own, side_a, side_b)
        rounded = jnp.concatenate([row.astype(jnp.bfloat16) for row in both], axis=1)
        back = jnp.dot(transposed[...], rounded, preferred_element_type=f32)
        for r in range(2):
            out[k, pl.ds(r, levels, stride=2), :] = (
                before[r] + back[:, r * width : (r + 1) * width]
            )
        pltpu.make_async_copy(out.at[k], far.at[k], sems.at[k]).start()
    for k in range(members):
        pltpu.make_async_copy(out.at[k], far.at[k], sems.at[k]).wait()


def per_device(ensemble, control, vertical, inverse_var, obs_code, obs_count):
    members, variables, levels, own_rows, width = ensemble.shape
    mem_size, grid_size = lax.axis_size("mem"), lax.axis_size("grid")
    factor = (members * mem_size) ** (-0.5)
    height = levels * own_rows
    half = mem_size // 2
    per_owner = levels // mem_size
    assert own_rows == 2 and per_owner * own_rows == 8
    mem_at, grid_at = lax.axis_index("mem"), lax.axis_index("grid")
    facts = [grid_at % 2 == 0, grid_at > 0, grid_at < grid_size - 1, mem_at % 2 == 0]
    facts = jnp.stack([x.astype(f32) for x in facts] + [(mem_at * per_owner).astype(f32)])
    place = jnp.broadcast_to(jnp.pad(facts, (0, 3))[:, None], (8, width))
    swap_a = [(i, i ^ 1) for i in range(grid_size)]
    swap_b = [(i, ((i + 1) ^ 1) - 1) for i in range(1, grid_size - 1)]
    cores = [[2 * i, 2 * i + 1] for i in range(half)]
    same_core = [[2 * i + c for i in range(half)] for c in range(2)]

    ens = ensemble.reshape(members, variables, height, width)
    ctl = control.reshape(members, height, width)
    meta_rows = 4 * obs_code.shape[0]

    field = jax.ShapeDtypeStruct((members * height, width), f32)
    wide = ctl.reshape(members * height, width).astype(f32)
    wide_a = lax.ppermute(wide, "grid", swap_a)
    wide_b = lax.ppermute(wide, "grid", swap_b)
    meta, weights = call(
        meta_kernel,
        (
            jax.ShapeDtypeStruct((meta_rows, width), f32),
            jax.ShapeDtypeStruct((variables * per_owner, width), f32),
        ),
        [ANY] + [VMEM] * 5,
    )(wide, place, inverse_var, obs_code, obs_count, ens)
    own_shape = jax.ShapeDtypeStruct((members, own_rows, levels, width), f32)
    own = call(own_kernel, own_shape, [VMEM] * 3)(place, wide, vertical)

    block = jax.ShapeDtypeStruct((half, variables, 8, width), f32)
    keep, send = call(
        functools.partial(partial_kernel, factor),
        (block, block),
        [VMEM, ANY] + [VMEM] * 5,
        [pltpu.VMEM((members, height, width), f32)],
    )(place, meta, own, wide_a, wide_b, vertical, ens)
    gathered = lax.all_gather(send, "mem", axis=0, axis_index_groups=cores)
    paired = call(pair_sum_kernel, block, [VMEM, VMEM, VMEM])(place, keep, gathered)
    paired, meta, place, weights = lax.optimization_barrier((paired, meta, place, weights))
    arrived = lax.all_to_all(paired, "mem", 0, 0, axis_index_groups=same_core, tiled=True)
    share = call(
        total_kernel, jax.ShapeDtypeStruct((variables * 8 + meta_rows, width), f32), [VMEM, VMEM]
    )(arrived, meta)

    share_a = lax.ppermute(share, "grid", swap_a)
    share_b = lax.ppermute(share, "grid", swap_b)
    spread = call(
        observe_kernel,
        block,
        [VMEM] * 5,
        [pltpu.VMEM((variables * 8, width), f32)],
    )(place, weights, share, share_b, share_a)
    mine = lax.all_to_all(spread, "mem", 0, 0, axis_index_groups=same_core, tiled=True)
    adjoint = lax.all_gather(mine, "mem", axis=0, axis_index_groups=cores)

    projected = call(
        functools.partial(project_kernel, factor),
        field,
        [VMEM, VMEM],
    )(adjoint, ens)
    projected_a = lax.ppermute(projected, "grid", swap_a)
    projected_b = lax.ppermute(projected, "grid", swap_b)
    own, turned = call(
        own_turned_kernel,
        (own_shape, jax.ShapeDtypeStruct(vertical.shape, vertical.dtype)),
        [VMEM] * 3,
    )(place, projected, vertical)
    whole = jax.ShapeDtypeStruct((members, height, width), f32)
    out = call(
        product_kernel,
        whole,
        [VMEM] + [VMEM] * 5,
        [pltpu.VMEM(whole.shape, f32), pltpu.SemaphoreType.DMA((members,))],
        out_spec=ANY,
    )(place, own, projected_a, projected_b, wide, turned)
    return out.reshape(control.shape)


def solution(mesh):
    return jax.shard_map(
        per_device,
        mesh=mesh,
        in_specs=(
            P("mem", None, None, "grid", None),
            P("mem", None, "grid", None),
            P(),
            P(),
            P("grid", None),
            P("grid", None),
        ),
        out_specs=P("mem", None, "grid", None),
        check_vma=False,
    )
```

```python
import functools
import jax
import jax.numpy as jnp
from jax import lax
from jax.experimental import pallas as pl
from jax.experimental.pallas import tpu as pltpu
from jax.sharding import PartitionSpec as P

diffusion = 0.2
near_weight = 0.75
far_weight = 0.25

VMEM = pl.BlockSpec(memory_space=pltpu.VMEM)
f32 = jnp.float32


ANY = pl.BlockSpec(memory_space=pl.ANY)


def call(body, out_shapes, in_specs, scratch=(), flops=1000000, out_spec=VMEM):
    return pl.pallas_call(
        body,
        out_shape=out_shapes,
        in_specs=list(in_specs),
        out_specs=jax.tree.map(lambda _: out_spec, out_shapes),
        scratch_shapes=list(scratch),
        compiler_params=pltpu.CompilerParams(vmem_limit_bytes=24 * 1024 * 1024),
        cost_estimate=pl.CostEstimate(flops=flops, bytes_accessed=1000000, transcendentals=0),
    )


def lanes(shape):
    return lax.broadcasted_iota(jnp.int32, shape, len(shape) - 1)


def from_left(x):
    return jnp.where(lanes(x.shape) == 0, 0.0, pltpu.roll(x, 1, x.ndim - 1))


def from_right(x):
    width = x.shape[-1]
    return jnp.where(lanes(x.shape) == width - 1, 0.0, pltpu.roll(x, width - 1, x.ndim - 1))


def smooth(row, up, down):
    pair = from_right(row) + from_left(row)
    return row + diffusion * (down + up + pair - 4.0 * row)


def smooth_twice(above, own, below, top, bottom):
    f_up = top * smooth(above[1], above[0], own[0])
    f_0 = smooth(own[0], above[1], own[1])
    f_1 = smooth(own[1], own[0], below[0])
    f_down = bottom * smooth(below[0], own[1], below[1])
    return smooth(f_0, f_up, f_1), smooth(f_1, f_0, f_down)


def own_part(own, top, bottom):
    zero = jnp.zeros_like(own[0])
    return smooth_twice((zero, zero), own, (zero, zero), top, bottom)


def halo_part(above, below, top, bottom):
    up = from_right(above[1]) + from_left(above[1])
    down = from_right(below[0]) + from_left(below[0])
    f_up = top * (above[1] + diffusion * (above[0] + up - 4.0 * above[1]))
    f_down = bottom * (below[0] + diffusion * (below[1] + down - 4.0 * below[0]))
    first = above[1] + diffusion * (up - 4.0 * above[1]) + f_up + diffusion * below[0]
    second = below[0] + diffusion * (down - 4.0 * below[0]) + f_down + diffusion * above[1]
    return diffusion * first, diffusion * second


def rows_of(ref, start, count):
    return [ref[pl.ds(start + r, count, stride=2), :] for r in range(2)]


def neighbours(even, a, b):
    keep = even > 0.5
    return [jnp.where(keep, y, x) for x, y in zip(a, b)], [jnp.where(keep, x, y) for x, y in zip(a, b)]


def flags_of(place):
    return [place[i : i + 1, :] for i in range(4)]


def mixed_rows(vertical, fields):
    width = fields[0].shape[1]
    side_by_side = jnp.concatenate([x.astype(jnp.bfloat16) for x in fields], axis=1)
    product = jnp.dot(vertical[...], side_by_side, preferred_element_type=f32)
    return [product[:, i * width : (i + 1) * width] for i in range(len(fields))]


def meta_kernel(after, place, inverse_var, code, count, ensemble, out, weights):
    values = inverse_var[...]
    variables = values.shape[0]
    per_owner = weights.shape[0] // variables
    lane = lanes(values.shape).astype(f32)
    for l in range(per_owner):
        picked = jnp.where(lane == place[4:5, :] + float(l), values, 0.0)
        weights[pl.ds(l, variables, stride=per_owner), :] = jnp.broadcast_to(
            jnp.sum(picked, axis=1, keepdims=True), values.shape
        )
    width = code.shape[1]
    source = lax.broadcasted_iota(jnp.int32, (width, width // 2), 0)
    target = lax.broadcasted_iota(jnp.int32, (width, width // 2), 1)
    n = code.shape[0]
    for i, what in enumerate((code, count)):
        values = what[...].astype(f32)
        for phase in range(2):
            pick = jnp.where(source == 2 * target + phase, 1.0, 0.0)
            out[pl.ds((2 * i + phase) * n, n), :] = jnp.dot(
                values, pick, preferred_element_type=f32, precision=lax.Precision.HIGHEST
            )


def own_kernel(place, control, vertical, out):
    members, _, levels = out.shape[:3]
    _, top, bottom, _ = flags_of(place)
    for k in range(members):
        rows = mixed_rows(vertical, rows_of(control, 2 * k * levels, levels))
        both = own_part(rows, top, bottom)
        for r in range(2):
            out[k, r] = both[r]


def own_turned_kernel(place, field, vertical, out, turned):
    turned[...] = vertical[...].astype(f32).T.astype(turned.dtype)
    members, _, levels = out.shape[:3]
    _, top, bottom, _ = flags_of(place)
    for k in range(members):
        both = own_part(rows_of(field, 2 * k * levels, levels), top, bottom)
        for r in range(2):
            out[k, r] = both[r]


def smoothed_rows(place, k, own, side_a, side_b, vertical=None):
    even, top, bottom, _ = flags_of(place)
    levels = own.shape[2]
    at = 2 * k * levels
    above, below = neighbours(even, rows_of(side_a, at, levels), rows_of(side_b, at, levels))
    if vertical is not None:
        rows = mixed_rows(vertical, above + below)
        above, below = rows[:2], rows[2:]
    both = halo_part(above, below, top, bottom)
    return [own[k, r] + both[r] for r in range(2)]


def partial_kernel(
    factor, place, after, own, side_a, side_b, vertical, ensemble, keep, send, local
):
    members, variables, height = ensemble.shape[:3]
    levels = height // 2
    for k in range(members):
        both = smoothed_rows(place, k, own, side_a, side_b, vertical)
        for r in range(2):
            local[k, pl.ds(r, levels, stride=2), :] = both[r]
    mine = flags_of(place)[3] > 0.5
    for j in range(keep.shape[0]):
        at = pl.ds(16 * j, 16)
        fields = [local[k, at, :] for k in range(members)]
        for v in range(variables):
            total = ensemble[0, v, at, :].astype(f32) * fields[0]
            for k in range(1, members):
                total = total + ensemble[k, v, at, :].astype(f32) * fields[k]
            total = factor * total
            keep[j, v] = jnp.where(mine, total[:8], total[8:])
            send[j, v] = jnp.where(mine, total[8:], total[:8])


def pair_sum_kernel(place, keep, gathered, out):
    first = flags_of(place)[3] > 0.5
    for j in range(out.shape[0]):
        out[j] = keep[j] + jnp.where(first, gathered[1, j], gathered[0, j])


def total_kernel(arrived, meta, out):
    total = arrived[0]
    for j in range(1, arrived.shape[0]):
        total = total + arrived[j]
    rows = 8 * total.shape[0]
    for v in range(total.shape[0]):
        out[8 * v : 8 * v + 8, :] = total[v]
    out[rows:, :] = meta[...]


def observe_kernel(place, weights, share, swap_b, pair_a, out, rows):
    even, top, bottom, _ = flags_of(place)
    height = rows.shape[0]
    n = height // 2
    own = rows_of(share, 0, n)
    keep_even = even > 0.5
    a = [
        jnp.where(keep_even, pair_a[1, pl.ds(r, n, stride=2), :], pair_a[0, pl.ds(r, n, stride=2), :])
        for r in range(2)
    ]
    above, below = neighbours(even, a, rows_of(swap_b, 0, n))
    u = dict(zip(range(-2, 4), above + own + below))

    def inside(f):
        return top if f < 0 else bottom if f > 3 else None

    def masked(x, f):
        scale = inside(f)
        return x if scale is None else x * scale

    fine = {}
    for f in range(-3, 7):
        a_row = f // 2
        other = a_row - 1 if f % 2 == 0 else a_row + 1
        line = near_weight * u[a_row] + far_weight * u[other]
        fine[f] = [
            masked(near_weight * line + far_weight * from_left(line), f),
            masked(near_weight * line + far_weight * from_right(line), f),
        ]
    meta_a = jnp.where(keep_even, pair_a[1, height:, :], pair_a[0, height:, :])
    wanted_above, wanted_below = neighbours(even, [meta_a], [swap_b[height:, :]])
    table = [wanted_above[0], share[height:, :], wanted_below[0]]

    def lookup(which, phase, f):
        block, line = (f + 4) // 4, f % 4
        at = (2 * which + phase) * 4 + line
        return table[block][at : at + 1, :]

    scale = weights[...]
    forcing, first, second, third, fourth = {}, {}, {}, {}, {}
    for f in range(-2, 6):
        e, o = fine[f]
        nexts = (o, from_right(e))
        previous = (from_left(o), e)
        for phase in range(2):
            code = lookup(0, phase, f)
            count = lookup(1, phase, f)
            m = [(code == float(which)).astype(f32) for which in range(1, 5)]
            diff = fine[f][phase] - m[0] * fine[f + 1][phase] - m[1] * fine[f - 1][phase]
            diff = diff - m[2] * nexts[phase] - m[3] * previous[phase]
            value = count * scale * diff
            forcing[f, phase] = value
            first[f, phase] = m[0] * value
            second[f, phase] = m[1] * value
            third[f, phase] = m[2] * value
            fourth[f, phase] = m[3] * value
    adjoint = {}
    for f in range(-1, 5):
        came_left = (from_left(third[f, 1]), third[f, 0])
        came_right = (fourth[f, 1], from_right(fourth[f, 0]))
        for phase in range(2):
            value = forcing[f, phase] - first[f - 1, phase] - second[f + 1, phase]
            adjoint[f, phase] = masked(value - came_left[phase] - came_right[phase], f)
    for a_row in range(2):
        f = 2 * a_row
        e, o = (
            near_weight * (adjoint[f, p] + adjoint[f + 1, p])
            + far_weight * (adjoint[f - 1, p] + adjoint[f + 2, p])
            for p in range(2)
        )
        result = near_weight * (e + o) + far_weight * (from_left(o) + from_right(e))
        rows[pl.ds(a_row, n, stride=2), :] = result
    for v in range(out.shape[1]):
        tile = rows[8 * v : 8 * v + 8, :]
        for j in range(out.shape[0]):
            out[j, v] = tile


def project_kernel(factor, adjoint, ensemble, out):
    members, variables, height = ensemble.shape[:3]
    for j in range(adjoint.shape[1]):
        at = pl.ds(16 * j, 16)
        for k in range(members):
            total = None
            for v in range(variables):
                wide = jnp.concatenate([adjoint[0, j, v], adjoint[1, j, v]], axis=0)
                term = ensemble[k, v, at, :].astype(f32) * wide
                total = term if total is None else total + term
            out[pl.ds(k * height + 16 * j, 16), :] = factor * total


def product_kernel(place, own, side_a, side_b, control, transposed, far, out, sems):
    members, _, levels, width = own.shape
    rounded = [
        row.astype(jnp.bfloat16)
        for k in range(members)
        for row in smoothed_rows(place, k, own, side_a, side_b)
    ]
    back = jnp.dot(
        transposed[...], jnp.concatenate(rounded, axis=1), preferred_element_type=f32
    )
    for k in range(members):
        before = rows_of(control, 2 * k * levels, levels)
        for r in range(2):
            at = (2 * k + r) * width
            out[k, pl.ds(r, levels, stride=2), :] = before[r] + back[:, at : at + width]
        pltpu.make_async_copy(out.at[k], far.at[k], sems.at[k]).start()
    for k in range(members):
        pltpu.make_async_copy(out.at[k], far.at[k], sems.at[k]).wait()


def per_device(ensemble, control, vertical, inverse_var, obs_code, obs_count):
    members, variables, levels, own_rows, width = ensemble.shape
    mem_size, grid_size = lax.axis_size("mem"), lax.axis_size("grid")
    factor = (members * mem_size) ** (-0.5)
    height = levels * own_rows
    half = mem_size // 2
    per_owner = levels // mem_size
    assert own_rows == 2 and per_owner * own_rows == 8
    mem_at, grid_at = lax.axis_index("mem"), lax.axis_index("grid")
    facts = [grid_at % 2 == 0, grid_at > 0, grid_at < grid_size - 1, mem_at % 2 == 0]
    facts = jnp.stack([x.astype(f32) for x in facts] + [(mem_at * per_owner).astype(f32)])
    place = jnp.broadcast_to(jnp.pad(facts, (0, 3))[:, None], (8, width))
    swap_a = [(i, i ^ 1) for i in range(grid_size)]
    swap_b = [(i, ((i + 1) ^ 1) - 1) for i in range(1, grid_size - 1)]
    pairs_a = [[2 * i, 2 * i + 1] for i in range(grid_size // 2)]
    cores = [[2 * i, 2 * i + 1] for i in range(half)]
    same_core = [[2 * i + c for i in range(half)] for c in range(2)]

    ens = ensemble.reshape(members, variables, height, width)
    ctl = control.reshape(members, height, width)
    meta_rows = 4 * obs_code.shape[0]

    field = jax.ShapeDtypeStruct((members * height, width), f32)
    wide = ctl.reshape(members * height, width).astype(f32)
    wide_a = lax.ppermute(wide, "grid", swap_a)
    wide_b = lax.ppermute(wide, "grid", swap_b)
    meta, weights = call(
        meta_kernel,
        (
            jax.ShapeDtypeStruct((meta_rows, width), f32),
            jax.ShapeDtypeStruct((variables * per_owner, width), f32),
        ),
        [ANY] + [VMEM] * 5,
    )(wide, place, inverse_var, obs_code, obs_count, ens)
    own_shape = jax.ShapeDtypeStruct((members, own_rows, levels, width), f32)
    own = call(own_kernel, own_shape, [VMEM] * 3)(place, wide, vertical)

    block = jax.ShapeDtypeStruct((half, variables, 8, width), f32)
    keep, send = call(
        functools.partial(partial_kernel, factor),
        (block, block),
        [VMEM, ANY] + [VMEM] * 5,
        [pltpu.VMEM((members, height, width), f32)],
    )(place, meta, own, wide_a, wide_b, vertical, ens)
    gathered = lax.all_gather(send, "mem", axis=0, axis_index_groups=cores)
    paired = call(pair_sum_kernel, block, [VMEM, VMEM, VMEM])(place, keep, gathered)
    paired, meta, place, weights = lax.optimization_barrier((paired, meta, place, weights))
    arrived = lax.all_to_all(paired, "mem", 0, 0, axis_index_groups=same_core, tiled=True)
    share = call(
        total_kernel, jax.ShapeDtypeStruct((variables * 8 + meta_rows, width), f32), [VMEM, VMEM]
    )(arrived, meta)

    share_b = lax.ppermute(share, "grid", swap_b)
    share_a = lax.all_gather(share, "grid", axis=0, axis_index_groups=pairs_a)
    spread = call(
        observe_kernel,
        block,
        [VMEM] * 5,
        [pltpu.VMEM((variables * 8, width), f32)],
    )(place, weights, share, share_b, share_a)
    mine = lax.all_to_all(spread, "mem", 0, 0, axis_index_groups=same_core, tiled=True)
    adjoint = lax.all_gather(mine, "mem", axis=0, axis_index_groups=cores)

    projected = call(
        functools.partial(project_kernel, factor),
        field,
        [VMEM, VMEM],
    )(adjoint, ens)
    projected_a = lax.ppermute(projected, "grid", swap_a)
    projected_b = lax.ppermute(projected, "grid", swap_b)
    own, turned = call(
        own_turned_kernel,
        (own_shape, jax.ShapeDtypeStruct(vertical.shape, vertical.dtype)),
        [VMEM] * 3,
    )(place, projected, vertical)
    whole = jax.ShapeDtypeStruct((members, height, width), f32)
    out = call(
        product_kernel,
        whole,
        [VMEM] + [VMEM] * 5,
        [pltpu.VMEM(whole.shape, f32), pltpu.SemaphoreType.DMA((members,))],
        out_spec=ANY,
    )(place, own, projected_a, projected_b, wide, turned)
    return out.reshape(control.shape)


def solution(mesh):
    return jax.shard_map(
        per_device,
        mesh=mesh,
        in_specs=(
            P("mem", None, None, "grid", None),
            P("mem", None, "grid", None),
            P(),
            P(),
            P("grid", None),
            P("grid", None),
        ),
        out_specs=P("mem", None, "grid", None),
        check_vma=False,
    )
```
